32 devices in a mesh: member: 2 (over x), tile: 16 (over z, y, core).
Axes of the slice: x: 2, y: 2, z: 4, core: 2. Of those that a mesh axis runs over, the one named last changes fastest.
Arguments:
- pressure: float32 [64, 128, 512], P('member', 'tile'), parts along dimension 0, may hold values from -1.5 to 1
- conductivity: float32 [64, 128, 512], P('member', 'tile'), parts along dimension 0, may hold values from 0.5 to 2
- soil_class: int32 [64, 128, 512], P('member', 'tile'), parts along dimension 0, may hold values from 0 to 11
- vg_alpha: float32 [12], replicated, may hold values from 0.3 to 2
- vg_shape: float32 [12], replicated, may hold values from 1.3 to 2.6
- bed: float32 [512, 256], P('tile', 'member'), parts along dimension 1, may hold values from -4 to 4
- flow_code: int32 [512, 256], P('tile', 'member'), parts along dimension 1, may hold values from 0 to 7
- surface_soil: int32 [512, 256], P('tile', 'member'), parts along dimension 1, may hold values from 0 to 11
- cover_class: int32 [512, 256], P('tile', 'member'), parts along dimension 1, may hold values from 0 to 16
- ponding: int32 [512, 256], P('tile', 'member'), parts along dimension 1, may hold values 0 or 1
- conveyance: float32 [17], replicated, may hold values from 0.3 to 3
- erodibility: float32 [12], replicated, may hold values from 0.1 to 1
Outputs:
- head_out: float32 [64, 128, 512], P('member', 'tile'), parts along dimension 0
- bed_out: float32 [512, 256], P('tile', 'member'), parts along dimension 1
The draws below stay inside these ranges and needn't reach their ends.
There are 2 independent parts, one for each index of `member`. The reference program is written for one: setup_inputs(seed, part) draws one part's arguments, and reference() takes and returns one part's arrays. A program takes and returns all parts, laid end to end along the dimension named above; an argument that names none is the same for every part. Nothing has to cross between parts.
All inputs are finite; a program needn't handle non-finite values. No bound on the sum of `ponding` on one device may be relied on, other than what follows from the above.
Results may differ from the reference program's by a relative error of at most 0.00035.
Values sent between devices are 32-bit elements; how exact they have to be, the bound alone decides.
A program may use at most 128 MiB of HBM per device.

```python
import math
import jax
import jax.numpy as jnp

LAYERS = 32
STEPS = 4
CLASSES = 12
COVERS = 17
NX = 128
NY = 512


def touch_ends(values, stream_key, smallest, high):
    spot = [jax.random.randint(jax.random.fold_in(stream_key, axis), (), 0, length) for axis, length in enumerate(values.shape)]
    widest = values.shape.index(max(values.shape))
    next_to = spot[:widest] + [(spot[widest] + 1) % values.shape[widest]] + spot[widest + 1:]
    return values.at[tuple(spot)].set(smallest).at[tuple(next_to)].set(high)


def levels(key, extent, shards, smallest, high):
    gain, own = 1.0, jax.random.fold_in(key, 6)
    for position, parts in shards:
        heights = jnp.exp(jax.random.uniform(jax.random.fold_in(own, position), (parts,), jnp.float32, smallest / len(shards), high / len(shards)))
        gain = gain * jnp.repeat(heights, extent[position] // parts).reshape([-1 if axis == position else 1 for axis in range(len(extent))])
    return gain


def bell_draw(key, extent, scale, limit, split=(), kind=jnp.bfloat16):
    drawn = scale * jax.random.normal(key, extent, jnp.float32)
    if split:
        drawn = drawn * levels(key, extent, split, -0.22, 0.18)
    return jnp.clip(drawn, -limit, limit).astype(kind)


def setup_inputs(seed: int = 0, part: int = 0) -> dict:
    streams_of = jax.random.split(jax.random.key(seed), 13)
    own_keys = jax.random.split(jax.random.fold_in(streams_of[12], part), 13)
    return {
        "pressure": jnp.clip(-1.5 + 2.5 * jax.random.uniform(own_keys[0], (LAYERS, NX, NY), jnp.float32) ** levels(own_keys[0], (LAYERS, NX, NY), ((1, 16),), -0.2, 0.2), -1.5, 1.0),
        "conductivity": jnp.clip(jnp.exp(math.log(2.0) - 1.3862944 * jax.random.uniform(own_keys[1], (LAYERS, NX, NY), jnp.float32) ** levels(own_keys[1], (LAYERS, NX, NY), ((1, 16),), -0.2, 0.2)), 0.5, 2.0),
        "soil_class": touch_ends(jax.random.randint(own_keys[2], (LAYERS, NX, NY), 0, CLASSES), jax.random.fold_in(own_keys[2], 1), 0, CLASSES - 1).astype(jnp.int32),
        "vg_alpha": jnp.clip(jnp.exp(jax.random.uniform(streams_of[3], (CLASSES,), jnp.float32, math.log(0.3), math.log(2.0))), 0.3, 2.0),
        "vg_shape": jnp.clip(jax.random.uniform(streams_of[4], (CLASSES,), jnp.float32, 1.3, 2.6), 1.3, 2.6),
        "bed": bell_draw(own_keys[5], (NY, NX), 1.0, 4.0, ((0, 16),), jnp.float32),
        "flow_code": touch_ends(jax.random.randint(own_keys[6], (NY, NX), 0, 8), jax.random.fold_in(own_keys[6], 1), 0, 7).astype(jnp.int32),
        "surface_soil": touch_ends(jax.random.randint(own_keys[7], (NY, NX), 0, CLASSES), jax.random.fold_in(own_keys[7], 1), 0, CLASSES - 1).astype(jnp.int32),
        "cover_class": touch_ends(jax.random.randint(own_keys[8], (NY, NX), 0, COVERS), jax.random.fold_in(own_keys[8], 1), 0, COVERS - 1).astype(jnp.int32),
        "ponding": touch_ends((jax.random.randint(own_keys[9], (NY, NX), 0, 4) < 1).astype(jnp.int32), jax.random.fold_in(own_keys[9], 1), 0, 1),
        "conveyance": jnp.clip(jnp.exp(jax.random.uniform(streams_of[10], (COVERS,), jnp.float32, math.log(0.3), math.log(3.0))), 0.3, 3.0),
        "erodibility": jnp.clip(jnp.exp(jax.random.uniform(streams_of[11], (CLASSES,), jnp.float32, math.log(0.1), math.log(1.0))), 0.1, 1.0),
    }


RELAX_STEP = 0.08
CAPACITY = 2.0
MIN_SLOPE = 0.01
BED_RATE = 2.0
SHIFT_X = (1, 1, 0, -1, -1, -1, 0, 1)
SHIFT_Y = (0, 1, 1, 1, 0, -1, -1, -1)

def retention(head, alpha_field, shape_field):
    exponent = 1.0 - 1.0 / shape_field
    suction = jnp.maximum(-head, 0.0)
    saturation = (1.0 + (alpha_field * suction) ** shape_field) ** (-exponent)
    inner = jnp.maximum(1.0 - saturation ** (1.0 / exponent), 0.0)
    permeab = jnp.sqrt(saturation) * (1.0 - inner ** exponent) ** 2
    return (saturation, permeab)

def relax(wide_head, wide_ks, wide_alpha, wide_shape):
    saturation, permeab = retention(wide_head, wide_alpha, wide_shape)
    conduct = wide_ks * permeab
    layers = wide_head.shape[0]
    height = wide_head - jnp.arange(layers, dtype=wide_head.dtype)[:, None, None]
    centre_k = conduct[:, 1:-1]
    centre_h = height[:, 1:-1]
    flow = 0.5 * (centre_k + conduct[:, 2:]) * (height[:, 2:] - centre_h)
    flow = flow + 0.5 * (centre_k + conduct[:, :-2]) * (height[:, :-2] - centre_h)
    side_k = jnp.pad(centre_k, ((0, 0), (0, 0), (1, 1)), mode='edge')
    side_h = jnp.pad(centre_h, ((0, 0), (0, 0), (1, 1)), mode='edge')
    flow = flow + 0.5 * (centre_k + side_k[:, :, 2:]) * (side_h[:, :, 2:] - centre_h)
    flow = flow + 0.5 * (centre_k + side_k[:, :, :-2]) * (side_h[:, :, :-2] - centre_h)
    vertical = 0.5 * (centre_k[:-1] + centre_k[1:]) * (centre_h[1:] - centre_h[:-1])
    zero_plane = jnp.zeros_like(vertical[:1])
    flow = flow + jnp.concatenate([vertical, zero_plane], 0) - jnp.concatenate([zero_plane, vertical], 0)
    drain = jnp.concatenate([jnp.zeros_like(centre_k[:-1]), centre_k[-1:]], 0)
    flow = flow - drain
    return wide_head[:, 1:-1] + RELAX_STEP * flow / (1.0 + CAPACITY * (1.0 - saturation[:, 1:-1]))

def surface_step(wide_bed, wide_depth, wide_coef, wide_erode, wide_code, rows, columns, flipped):

    def window(field, first, second):
        return field[1 + first:rows + 3 + first, 1 + second:columns + 3 + second]

    def source(field, first, second):
        return field[1 - first:rows + 1 - first, 1 - second:columns + 1 - second]
    shifts = []
    for course in range(8):
        if flipped:
            shifts.append((SHIFT_X[course], SHIFT_Y[course]))
        else:
            shifts.append((SHIFT_Y[course], SHIFT_X[course]))
    centre = window(wide_bed, 0, 0)
    codes = window(wide_code, 0, 0)
    slope = jnp.full_like(centre, MIN_SLOPE)
    for course in range(8):
        first, second = shifts[course]
        distance = math.sqrt(first * first + second * second)
        drop = jnp.maximum(centre - window(wide_bed, first, second), 0.0) / distance
        slope = slope + jnp.where(codes == course, drop, 0.0)
    depth = window(wide_depth, 0, 0)
    root_slope = jnp.sqrt(slope)
    drive = window(wide_coef, 0, 0) * root_slope * depth ** (2.0 / 3.0)
    outflow = depth * drive / (1.0 + drive)
    sediment = window(wide_erode, 0, 0) * outflow * root_slope
    inflow = jnp.zeros_like(outflow[1:rows + 1, 1:columns + 1])
    sed_in = jnp.zeros_like(inflow)
    for course in range(8):
        first, second = shifts[course]
        chosen = source(codes, first, second) == course
        inflow = inflow + jnp.where(chosen, source(outflow, first, second), 0.0)
        sed_in = sed_in + jnp.where(chosen, source(sediment, first, second), 0.0)
    change = inflow - outflow[1:rows + 1, 1:columns + 1]
    bed_change = BED_RATE * (sed_in - sediment[1:rows + 1, 1:columns + 1])
    return (change, bed_change)

def reference(pressure, conductivity, soil_class, vg_alpha, vg_shape, bed, flow_code, surface_soil, cover_class, ponding, conveyance, erodibility):
    alpha_field = vg_alpha[soil_class]
    shape_field = vg_shape[soil_class]
    coef = conveyance[cover_class] * (1.0 - ponding.astype(jnp.float32))
    erode = erodibility[surface_soil]
    codes = flow_code.astype(jnp.float32)
    xpad = ((0, 0), (1, 1), (0, 0))
    ks_wide = jnp.pad(conductivity, xpad, mode='edge')
    alpha_wide = jnp.pad(alpha_field, xpad, mode='edge')
    shape_wide = jnp.pad(shape_field, xpad, mode='edge')
    coef_wide = jnp.pad(coef, 2)
    erode_wide = jnp.pad(erode, 2)
    code_wide = jnp.pad(codes, 2)
    head = pressure
    level = bed
    for section_index in range(STEPS):
        for sweep_index in range(2):
            head = relax(jnp.pad(head, xpad, mode='edge'), ks_wide, alpha_wide, shape_wide)
        depth = jnp.maximum(head[0].T, 0.0)
        change, bed_change = surface_step(jnp.pad(level, 2), jnp.pad(depth, 2), coef_wide, erode_wide, code_wide, NY, NX, False)
        head = head.at[0].add(change.T)
        level = level + bed_change
    return (head, level)
```

```python
import functools
import math

import jax
import jax.numpy as jnp
from jax import lax
from jax.experimental import pallas as pl
from jax.experimental.pallas import tpu as pltpu
from jax.sharding import PartitionSpec as P

STEPS = 4
RELAX_STEP = 0.08
CAPACITY = 2.0
MIN_SLOPE = 0.01
BED_RATE = 2.0
SHIFT_X = (1, 1, 0, -1, -1, -1, 0, 1)
SHIFT_Y = (0, 1, 1, 1, 0, -1, -1, -1)
TINY = 1.2e-38
LANES = 128
KINDS = 9
TOPS, REST, FLUX, LEVEL, DEPTH, SOIL_K, SOIL_C, TOP_K, TOP_C = range(KINDS)
HALO = 2
TOP = 8
EDGE = 4


def table_pick(classes, table, entries):
    picked = jnp.full(classes.shape, table(0), jnp.float32)
    for entry in range(1, entries):
        picked = jnp.where(classes == entry, table(entry), picked)
    return picked


def turn(values, shift, axis):
    shift = shift % values.shape[axis]
    return values if shift == 0 else pltpu.roll(values, shift, axis)


def kernel(
    count,
    rows,
    head_hbm,
    ks_hbm,
    class_hbm,
    alpha_hbm,
    shape_hbm,
    bed_hbm,
    code_hbm,
    soil_hbm,
    cover_hbm,
    pond_hbm,
    convey_hbm,
    erod_hbm,
    head_out,
    bed_out,
    head_in,
    ks_in,
    class_in,
    alpha_t,
    shape_t,
    bed_in,
    code_in,
    soil_in,
    cover_in,
    pond_in,
    convey_t,
    erod_t,
    load_sem,
    head_a,
    head_b,
    k_a,
    k_b,
    gain,
    ks,
    alpha,
    shape,
    half_m,
    top_k,
    top_soil,
    levels,
    depths,
    maps,
    class_out,
    class_halo,
    class_top,
    tops,
    rest,
    flux_out,
    flux,
    edge,
    edges,
    halo_change,
    packed,
    gathered,
    final_src,
    final_dst,
    turned,
    send_sem,
    recv_sem,
    spread_send,
    spread_recv,
    final_send,
    final_recv,
):
    layers = head_hbm.shape[0] // rows
    columns = head_hbm.shape[1]
    strip = bed_in.shape[0]
    width = bed_in.shape[1]
    per = LANES // strip
    groups = columns // LANES
    tiles = layers // TOP
    me = lax.axis_index("tile")
    half = rows // 2
    whole_part = slice(0, layers)
    top_part = slice(0, TOP)
    rest_part = slice(TOP, layers)

    def at(tile):
        return {"tile": tile}

    def exists(side):
        other = me + 2 * side - 1
        return jnp.logical_and(other >= 0, other < count)

    def copy_to(kind, slot, side, src, dst):
        return pltpu.make_async_remote_copy(
            src_ref=src,
            dst_ref=dst,
            send_sem=send_sem.at[kind, slot, side],
            recv_sem=recv_sem.at[kind, slot, 1 - side],
            device_id=at(me + 2 * side - 1),
            device_id_type=pl.DeviceIdType.MESH,
        )

    def push(kind, slot, side, src, dst):
        copy_to(kind, slot, side, src, dst).start()

    def got(kind, slot, side, ref):
        copy_to(kind, slot, 1 - side, ref, ref).wait_recv()

    def sent(kind, slot, side, ref):
        copy_to(kind, slot, side, ref, ref).wait_send()

    barrier = pltpu.get_barrier_semaphore()
    for away in range(1, count):
        pl.semaphore_signal(
            barrier,
            inc=1,
            device_id=at(lax.rem(me + away, count)),
            device_id_type=pl.DeviceIdType.MESH,
        )

    loads = [
        pltpu.make_async_copy(
            source.at[:, group * LANES : (group + 1) * LANES],
            target.at[group],
            load_sem.at[index, group],
        )
        for index, (source, target) in enumerate(
            ((head_hbm, head_in), (class_hbm, class_in), (ks_hbm, ks_in))
        )
        for group in range(groups)
    ]
    wide_loads = len(loads)
    loads += [
        pltpu.make_async_copy(source, target, load_sem.at[3, index])
        for index, (source, target) in enumerate(
            (
                (alpha_hbm, alpha_t),
                (shape_hbm, shape_t),
                (cover_hbm, cover_in),
                (pond_hbm, pond_in),
                (soil_hbm, soil_in),
                (code_hbm, code_in),
                (bed_hbm, bed_in),
                (convey_hbm, convey_t),
                (erod_hbm, erod_t),
            )
        )
    ]
    for load in loads:
        load.start()

    levels[...] = jnp.zeros_like(levels)
    depths[...] = jnp.zeros_like(depths)
    edge[...] = jnp.zeros_like(edge)
    edges[...] = jnp.zeros_like(edges)
    halo_change[...] = jnp.zeros_like(halo_change)

    def soil(found):
        scale = lax.log2(table_pick(found, lambda i: alpha_t[i], alpha_t.shape[0]))
        bend = table_pick(found, lambda i: shape_t[i], shape_t.shape[0])
        return scale, bend, 0.5 / bend - 0.5

    def soil_tile(row, part, found):
        alpha[row, part], shape[row, part], half_m[row, part] = soil(found)

    def conduct(head, scale, bend, power, full_k):
        log_a = lax.log2(jnp.maximum(-head, TINY)) + scale
        log_p = bend * log_a
        log_w = lax.log2(1.0 + lax.exp2(log_p))
        root = lax.exp2(power * log_w)
        full = root * root
        inner = 1.0 - lax.exp2(log_p - log_a) * full
        return full_k * root * (inner * inner), full

    def conduct_row(head, k_ref, row, part, gains=True):
        for tile in range(part.start // TOP, part.stop // TOP):
            spot = slice(tile * TOP, (tile + 1) * TOP)
            k, full = conduct(
                head[row, spot], alpha[row, spot], shape[row, spot], half_m[row, spot], ks[row, spot]
            )
            k_ref[row, spot] = k
            if gains:
                gain[row, spot] = RELAX_STEP / (1.0 + CAPACITY * (1.0 - full))

    layer = lax.broadcasted_iota(jnp.int32, (TOP, columns), 0)
    top_edge = layer == 0
    low_edge = layer == TOP - 1
    last_lane = lax.broadcasted_iota(jnp.int32, (TOP, LANES), 1) == LANES - 1
    body = columns - LANES

    def side_flow(h, k):
        right = (k + turn(k, -1, 1)) * (turn(h, -1, 1) - h)
        right = jnp.concatenate(
            [right[:, :body], jnp.where(last_lane, 0.0, right[:, body:])], axis=1
        )
        return right - turn(right, 1, 1)

    def faces(src, k_ref, row, others):
        def flow(spot, h, k):
            total = None
            for other in others:
                term = (k + k_ref[other, spot]) * (src[other, spot] - h)
                total = term if total is None else total + term
            return total

        return flow

    def flow_row(src, dst, k_ref, row, across, count_tiles=None):
        shown = tiles if count_tiles is None else count_tiles
        spots = [slice(t * TOP, (t + 1) * TOP) for t in range(shown)]
        hs = [src[row, spot] for spot in spots]
        k_s = [k_ref[row, spot] for spot in spots]
        up_h = [turn(h, -1, 0) for h in hs]
        up_k = [turn(k, -1, 0) for k in k_s]
        before = None
        for tile in range(shown):
            h, k, spot = hs[tile], k_s[tile], spots[tile]
            if tile < shown - 1:
                below_h = jnp.where(low_edge, up_h[tile + 1], up_h[tile])
                below_k = jnp.where(low_edge, up_k[tile + 1], up_k[tile])
                down = (k + below_k) * (below_h - h - 1.0)
            else:
                down = (k + up_k[tile]) * (up_h[tile] - h - 1.0)
                if shown == tiles:
                    down = jnp.where(low_edge, -2.0 * k, down)
            turned_down = turn(down, 1, 0)
            came = jnp.where(top_edge, 0.0 if before is None else before, turned_down)
            before = turned_down
            flow = across(spot, h, k) + side_flow(h, k) + (down - came)
            result = h + flow * gain[row, spot]
            if dst is None:
                return result[0:1]
            dst[row, spot] = result

    def strided(ref, row, tile):
        spot = pl.ds(tile * TOP * rows + row, TOP, stride=rows)
        return jnp.concatenate([ref[group, spot, :] for group in range(groups)], axis=1)

    def bring(row):
        for tile in range(tiles):
            spot = slice(tile * TOP, (tile + 1) * TOP)
            head_a[row + 1, spot] = strided(head_in, row, tile)
            ks[row + 1, spot] = 0.5 * strided(ks_in, row, tile)

    def bring_soil(row):
        for tile in range(tiles):
            spot = slice(tile * TOP, (tile + 1) * TOP)
            soil_tile(row + 1, spot, strided(class_in, row, tile))

    edge_rows = (0, 1, rows - 2, rows - 1)
    for load in loads[:wide_loads]:
        load.wait()
    for place, row in enumerate(edge_rows):
        bring(row)
        for tile in range(tiles):
            class_out[place, tile * TOP : (tile + 1) * TOP] = strided(class_in, row, tile)

    pl.semaphore_wait(barrier, count - 1)

    far = lax.rem(me, 2)

    def both_sides(work):
        for first in range(2):

            @pl.when(far == first)
            def _():
                work(first)
                work(1 - first)

    def edge_of(side):
        return 1 + side * (rows - 1), 1 - 2 * side

    def face_flux(side):
        own, step = edge_of(side)
        conduct_row(head_a, k_a, own, rest_part)
        conduct_row(head_a, k_a, own + step, rest_part)
        for tile in range(1, tiles):
            spot = slice(tile * TOP, (tile + 1) * TOP)
            flux_out[side, (tile - 1) * TOP : tile * TOP] = (
                k_a[own, spot] + k_a[own + step, spot]
            ) * (head_a[own + step, spot] - head_a[own, spot])

    def start_side(side):
        there = 1 - side
        own_row, inward = edge_of(side)
        low = 1 + side * (rows - 2)

        @pl.when(exists(side))
        def _():
            push(TOPS, 0, side, head_a.at[pl.ds(low, 2), top_part], tops.at[0, there])
            push(REST, 0, side, head_a.at[own_row, rest_part], rest.at[0, there])
            push(SOIL_C, 0, side, class_out.at[3 * side], class_halo.at[there])
            push(SOIL_K, 0, side, ks.at[own_row], ks.at[(rows + 1) * there])
            push(TOP_C, 0, side, class_out.at[1 + side, top_part], class_top.at[there])
            push(TOP_K, 0, side, ks.at[own_row + inward, top_part], top_k.at[1, there])

    both_sides(start_side)

    for load in loads[wide_loads : wide_loads + 2]:
        load.wait()
    for row in edge_rows:
        bring_soil(row)

    def start_flux(side):
        face_flux(side)

        @pl.when(exists(side))
        def _():
            push(FLUX, 0, side, flux_out.at[side], flux.at[0, 1 - side])

    both_sides(start_flux)

    for load in loads[wide_loads + 2 :]:
        load.wait()
    coef_y = table_pick(cover_in[...], lambda i: convey_t[i], convey_t.shape[0]) * (
        1.0 - pond_in[...].astype(jnp.float32)
    )
    erode_y = table_pick(soil_in[...], lambda i: erod_t[i], erod_t.shape[0])
    stacked = jnp.concatenate(
        [coef_y, erode_y, code_in[...].astype(jnp.float32), bed_in[...]], axis=0
    )
    packed[0:rows] = jnp.zeros((rows, LANES), jnp.float32)
    packed[rows + width : 2 * rows + width] = jnp.zeros((rows, LANES), jnp.float32)
    for block in range(width // LANES):
        packed[rows + block * LANES : rows + (block + 1) * LANES] = jnp.transpose(
            stacked[:, block * LANES : (block + 1) * LANES]
        )

    def spread(away):
        peer = lax.rem(me + away, count)
        return pltpu.make_async_remote_copy(
            src_ref=packed.at[pl.ds(pl.multiple_of(peer * rows, rows), 3 * rows)],
            dst_ref=gathered.at[me],
            send_sem=spread_send.at[away],
            recv_sem=spread_recv.at[away],
            device_id=at(peer),
            device_id_type=pl.DeviceIdType.MESH,
        )

    for away in range(1, count):
        spread(away).start()
    gathered[me] = packed[pl.ds(pl.multiple_of(me * rows, rows), 3 * rows)]

    own = slice(rows, 2 * rows)
    wide_lane = lax.broadcasted_iota(jnp.int32, (3 * rows, columns), 1)
    piece = lax.broadcasted_iota(jnp.int32, (3 * rows, LANES), 1) // strip

    def assemble():
        for away in range(1, count):
            spread(away).wait()
        for group in range(groups):
            for kind in range(4):
                joined = None
                for part in range(per):
                    block = turn(gathered[group * per + part], (part - kind) * strip, 1)
                    joined = block if joined is None else jnp.where(piece == part, block, joined)
                spot = slice(group * LANES, (group + 1) * LANES)
                if kind < 3:
                    maps[kind, :, spot] = joined
                else:
                    levels[0, :, spot] = joined

    def shifted(values, first, second):
        values = turn(values, -second, 1)
        if second == 1:
            values = jnp.where(wide_lane == columns - 1, 0.0, values)
        if second == -1:
            values = jnp.where(wide_lane == 0, 0.0, values)
        return turn(values, -first, 0)

    def surface(level, depth):
        coef, erode, code = maps[0], maps[1], maps[2]
        target = jnp.zeros_like(level)
        scale = jnp.ones_like(level)
        for course in range(8):
            first, second = SHIFT_X[course], SHIFT_Y[course]
            chosen = code == course
            target = jnp.where(chosen, shifted(level, first, second), target)
            if first * second != 0:
                scale = jnp.where(chosen, 1.0 / math.sqrt(2.0), scale)
        slope = MIN_SLOPE + jnp.maximum(level - target, 0.0) * scale
        root = jnp.sqrt(slope)
        power = lax.exp2((2.0 / 3.0) * lax.log2(jnp.maximum(depth, TINY)))
        drive = coef * root * power
        outflow = depth * drive / (1.0 + drive)
        sediment = erode * outflow * root
        sums = []
        for field in (outflow, sediment):
            total = -field
            for course in range(8):
                sent_on = jnp.where(code == course, field, 0.0)
                total = total + shifted(sent_on, -SHIFT_X[course], -SHIFT_Y[course])
            sums.append(total)
        return sums[0], BED_RATE * sums[1]

    for row in range(2, rows - 2):
        bring(row)
        bring_soil(row)
        conduct_row(head_a, k_a, row + 1, rest_part)

    @pl.loop(0, STEPS)
    def _(step):
        slot = lax.rem(step, 2)
        other = 1 - slot
        going = step < STEPS - 1

        for row in range(1, rows + 1):
            conduct_row(head_a, k_a, row, top_part)

        def side_work(side):
            there = 1 - side
            own_row, inward = edge_of(side)
            halo = own_row - inward
            here = exists(side)
            outer = jnp.where(here, halo, own_row)
            second = own_row + inward
            third = second + inward

            for ahead in range(1, half):
                row = own_row + ahead * inward
                flow_row(
                    head_a, head_b, k_a, row, faces(head_a, k_a, row, (row - inward, row + inward))
                )
            conduct_row(head_b, k_b, second, whole_part)
            conduct_row(head_b, k_b, third, whole_part)
            conduct_row(head_b, k_b, third + inward, top_part)

            @pl.when(jnp.logical_and(here, step == 0))
            def _():
                got(SOIL_C, 0, side, class_halo.at[side])
                got(TOP_C, 0, side, class_top.at[side])
                got(SOIL_K, 0, side, ks.at[halo])
                got(TOP_K, 0, side, top_k.at[1, side])
                sent(SOIL_C, 0, side, class_halo.at[side])
                sent(TOP_C, 0, side, class_top.at[side])
                sent(SOIL_K, 0, side, ks.at[halo])
                sent(TOP_K, 0, side, top_k.at[1, side])
                sent(TOPS, 0, side, tops.at[0, side])
                for tile in range(tiles):
                    spot = slice(tile * TOP, (tile + 1) * TOP)
                    soil_tile(halo, spot, class_halo[side, spot])
                a, b, c = soil(class_top[side])
                top_soil[0, side], top_soil[1, side], top_soil[2, side] = a, b, c

            @pl.when(here)
            def _():
                got(TOPS, slot, side, tops.at[slot, side])
                got(REST, slot, side, rest.at[slot, side])

            head_a[halo, top_part] = tops[slot, side, there]
            head_a[halo, 0:1] = head_a[halo, 0:1] + halo_change[side, 0:1]
            tops[slot, side, side, 0:1] = tops[slot, side, side, 0:1] + halo_change[side, 1:2]
            head_a[halo, rest_part] = rest[slot, side]
            conduct_row(head_a, k_a, halo, whole_part)
            beyond_h = tops[slot, side, side]
            beyond_k, _unused = conduct(
                beyond_h, top_soil[0, side], top_soil[1, side], top_soil[2, side], top_k[1, side]
            )
            top_k[2, side] = beyond_k

            flow_row(
                head_a, head_b, k_a, own_row, faces(head_a, k_a, own_row, (outer, second))
            )
            conduct_row(head_b, k_b, own_row, whole_part)
            flow_row(
                head_b, head_a, k_b, second, faces(head_b, k_b, second, (own_row, third))
            )
            third_top = flow_row(
                head_b,
                None,
                k_b,
                third,
                faces(head_b, k_b, third, (second, third + inward)),
                count_tiles=1,
            )
            edge[side, 2:3] = jnp.maximum(third_top, 0.0)
            edge[side, 1:2] = jnp.maximum(head_a[second, 0:1], 0.0)

            @pl.when(here)
            def _():
                got(FLUX, slot, side, flux.at[slot, side])
                sent(FLUX, slot, side, flux.at[slot, side])
                sent(REST, slot, side, rest.at[slot, side])

            def halo_faces(spot, h, k):
                inner = (k + k_a[own_row, spot]) * (head_a[own_row, spot] - h)
                if spot.start == 0:
                    return inner + (k + top_k[2, side]) * (tops[slot, side, side] - h)
                return inner + flux[slot, side, spot.start - TOP : spot.stop - TOP]

            flow_row(head_a, head_b, k_a, halo, halo_faces)
            conduct_row(head_b, k_b, halo, whole_part, gains=False)
            flow_row(
                head_b, head_a, k_b, own_row, faces(head_b, k_b, own_row, (outer, second))
            )
            edge[side, 0:1] = jnp.maximum(head_a[own_row, 0:1], 0.0)

            @pl.when(here)
            def _():
                push(DEPTH, other, side, edge.at[side], edges.at[other, there])

            @pl.when(jnp.logical_and(here, going))
            def _():
                low = 1 + side * (rows - 2)
                push(
                    TOPS, other, side, head_a.at[pl.ds(low, 2), top_part], tops.at[other, there]
                )
                push(REST, other, side, head_a.at[own_row, rest_part], rest.at[other, there])

            @pl.when(going)
            def _():
                face_flux(side)

            @pl.when(jnp.logical_and(here, going))
            def _():
                push(FLUX, other, side, flux_out.at[side], flux.at[other, there])

        both_sides(side_work)

        for row in (half, half + 1):
            conduct_row(head_b, k_b, row, rest_part)
        for row in range(3, rows - 1):
            flow_row(head_b, head_a, k_b, row, faces(head_b, k_b, row, (row - 1, row + 1)))

        @pl.when(going)
        def _():
            for row in range(3, rows - 1):
                conduct_row(head_a, k_a, row, rest_part)

        @pl.when(step == 0)
        def _():
            assemble()

        for row in range(rows):
            depths[rows + row : rows + row + 1] = jnp.maximum(head_a[row + 1, 0:1, :], 0.0)

        for side in range(2):

            @pl.when(jnp.logical_and(exists(side), step > 0))
            def _():
                spot = slice(2 * rows * side, 2 * rows * side + rows)
                got(LEVEL, slot, side, levels.at[slot, spot])
                sent(LEVEL, slot, side, levels.at[slot, spot])

        for side in range(2):

            @pl.when(exists(side))
            def _():
                got(DEPTH, other, side, edges.at[other, side])
                sent(DEPTH, other, side, edges.at[other, side])

        for away in range(3):
            spot = rows - 1 - away
            depths[spot : spot + 1] = edges[other, 0, away : away + 1]
            spot = 2 * rows + away
            depths[spot : spot + 1] = edges[other, 1, away : away + 1]

        change, bed_change = surface(levels[slot], depths[...])

        for side in range(2):

            @pl.when(jnp.logical_and(exists(side), going))
            def _():
                sent(TOPS, other, side, tops.at[other, side])

        for row in range(rows):
            spot = rows + row
            head_a[row + 1, 0:1, :] = head_a[row + 1, 0:1, :] + change[spot : spot + 1]
        for away in range(2):
            spot = rows - 1 - away
            halo_change[0, away : away + 1] = change[spot : spot + 1]
            spot = 2 * rows + away
            halo_change[1, away : away + 1] = change[spot : spot + 1]
        levels[other, own] = levels[slot, own] + bed_change[own]

        for side in range(2):

            @pl.when(jnp.logical_and(exists(side), going))
            def _():
                spot = slice(2 * rows * (1 - side), 2 * rows * (1 - side) + rows)
                push(LEVEL, other, side, levels.at[other, own], levels.at[other, spot])

    for group in range(groups):
        final_src[group] = levels[STEPS % 2, own, group * LANES : (group + 1) * LANES]

    def finish(away):
        peer = lax.rem(me + away, count)
        return pltpu.make_async_remote_copy(
            src_ref=final_src.at[peer // per],
            dst_ref=final_dst.at[me],
            send_sem=final_send.at[away],
            recv_sem=final_recv.at[away],
            device_id=at(peer),
            device_id_type=pl.DeviceIdType.MESH,
        )

    for away in range(1, count):
        finish(away).start()
    final_dst[me] = final_src[me // per]
    for row in range(rows):
        for tile in range(tiles):
            for group in range(groups):
                start = (tile * TOP * groups + group) * rows + row
                head_out[pl.ds(start, TOP, stride=groups * rows), :] = head_a[
                    row + 1,
                    tile * TOP : (tile + 1) * TOP,
                    group * LANES : (group + 1) * LANES,
                ]
    for away in range(1, count):
        finish(away).wait()
    members = LANES // rows
    for block in range(width // LANES):
        part = final_dst[block * members : (block + 1) * members]
        turned[:, block * LANES : (block + 1) * LANES] = jnp.transpose(
            part.reshape(LANES, LANES)
        )
    start = pl.multiple_of(lax.rem(me, per) * strip, strip)
    bed_out[...] = turned[pl.ds(start, strip)]


def on_device(
    pressure,
    conductivity,
    soil_class,
    vg_alpha,
    vg_shape,
    bed,
    flow_code,
    surface_soil,
    cover_class,
    ponding,
    conveyance,
    erodibility,
):
    count = lax.axis_size("tile")
    layers, rows, columns = pressure.shape
    strip, width = bed.shape
    groups = columns // LANES
    head = pressure.reshape(layers * rows, columns)
    ks = conductivity.reshape(layers * rows, columns)
    classes = soil_class.reshape(layers * rows, columns)
    vmem = pl.BlockSpec(memory_space=pltpu.VMEM)
    hbm = pl.BlockSpec(memory_space=pltpu.HBM)
    pin = lambda x: pltpu.with_memory_space_constraint(x, pltpu.HBM)
    wide = pltpu.VMEM((rows + 2, layers, columns), jnp.float32)
    dma = pltpu.SemaphoreType.DMA
    head_out, bed_out = pl.pallas_call(
        functools.partial(kernel, count, rows),
        out_shape=(
            jax.ShapeDtypeStruct((layers * rows * groups, LANES), jnp.float32),
            jax.ShapeDtypeStruct((strip, width), jnp.float32),
        ),
        in_specs=[hbm] * 12,
        out_specs=(vmem, vmem),
        scratch_shapes=[
            pltpu.VMEM((groups, layers * rows, LANES), jnp.float32),
            pltpu.VMEM((groups, layers * rows, LANES), jnp.float32),
            pltpu.VMEM((groups, layers * rows, LANES), jnp.int32),
            pltpu.SMEM(vg_alpha.shape, jnp.float32),
            pltpu.SMEM(vg_shape.shape, jnp.float32),
            pltpu.VMEM(bed.shape, jnp.float32),
            pltpu.VMEM(bed.shape, jnp.int32),
            pltpu.VMEM(bed.shape, jnp.int32),
            pltpu.VMEM(bed.shape, jnp.int32),
            pltpu.VMEM(bed.shape, jnp.int32),
            pltpu.SMEM(conveyance.shape, jnp.float32),
            pltpu.SMEM(erodibility.shape, jnp.float32),
            dma((4, max(groups, 9))),
            wide,
            wide,
            wide,
            wide,
            wide,
            wide,
            wide,
            wide,
            wide,
            pltpu.VMEM((3, 2, TOP, columns), jnp.float32),
            pltpu.VMEM((3, 2, TOP, columns), jnp.float32),
            pltpu.VMEM((2, 3 * rows, columns), jnp.float32),
            pltpu.VMEM((3 * rows, columns), jnp.float32),
            pltpu.VMEM((3, 3 * rows, columns), jnp.float32),
            pltpu.VMEM((4, layers, columns), jnp.int32),
            pltpu.VMEM((2, layers, columns), jnp.int32),
            pltpu.VMEM((2, TOP, columns), jnp.int32),
            pltpu.VMEM((2, 2, 2, TOP, columns), jnp.float32),
            pltpu.VMEM((2, 2, layers - TOP, columns), jnp.float32),
            pltpu.VMEM((2, layers - TOP, columns), jnp.float32),
            pltpu.VMEM((2, 2, layers - TOP, columns), jnp.float32),
            pltpu.VMEM((2, EDGE, columns), jnp.float32),
            pltpu.VMEM((2, 2, EDGE, columns), jnp.float32),
            pltpu.VMEM((2, EDGE, columns), jnp.float32),
            pltpu.VMEM((width + 2 * rows, LANES), jnp.float32),
            pltpu.VMEM((count, 3 * rows, LANES), jnp.float32),
            pltpu.VMEM((columns // LANES, rows, LANES), jnp.float32),
            pltpu.VMEM((count, rows, LANES), jnp.float32),
            pltpu.VMEM((LANES, width), jnp.float32),
            dma((KINDS, 2, 2)),
            dma((KINDS, 2, 2)),
            dma((count,)),
            dma((count,)),
            dma((count,)),
            dma((count,)),
        ],
        compiler_params=pltpu.CompilerParams(
            collective_id=0, has_side_effects=True, vmem_limit_bytes=40 * 1024 * 1024
        ),
    )(
        pin(head),
        pin(ks),
        pin(classes),
        pin(vg_alpha),
        pin(vg_shape),
        pin(bed),
        pin(flow_code),
        pin(surface_soil),
        pin(cover_class),
        pin(ponding),
        pin(conveyance),
        pin(erodibility),
    )
    head_out = jnp.swapaxes(head_out.reshape(layers, groups, rows, LANES), 1, 2)
    return head_out.reshape(layers, rows, columns), bed_out


def solution(mesh):
    in_specs = (
        P("member", "tile", None),
        P("member", "tile", None),
        P("member", "tile", None),
        P(),
        P(),
        P("tile", "member"),
        P("tile", "member"),
        P("tile", "member"),
        P("tile", "member"),
        P("tile", "member"),
        P(),
        P(),
    )
    out_specs = (P("member", "tile", None), P("tile", "member"))
    return jax.shard_map(
        on_device, mesh=mesh, in_specs=in_specs, out_specs=out_specs, check_vma=False
    )
```

```python
import functools
import math

import jax
import jax.numpy as jnp
from jax import lax
from jax.experimental import pallas as pl
from jax.experimental.pallas import tpu as pltpu
from jax.sharding import PartitionSpec as P

STEPS = 4
RELAX_STEP = 0.08
CAPACITY = 2.0
GAIN_BASE = (1.0 + CAPACITY) / RELAX_STEP
GAIN_SLOPE = CAPACITY / RELAX_STEP
MIN_SLOPE = 0.01
BED_RATE = 2.0
SHIFT_X = (1, 1, 0, -1, -1, -1, 0, 1)
SHIFT_Y = (0, 1, 1, 1, 0, -1, -1, -1)
TINY = 1.2e-38
LANES = 128
KINDS = 11
TOPS, REST, FLUX, LEVEL, DEPTH, HEAD, SOIL_K, SOIL_C, TOP_K, TOP_C, MAPS = range(KINDS)
HALO = 2
TOP = 8
EDGE = 4


def table_pick(classes, table, entries):
    picked = jnp.full(classes.shape, table(0), jnp.float32)
    for entry in range(1, entries):
        picked = jnp.where(classes == entry, table(entry), picked)
    return picked


def turn(values, shift, axis):
    shift = shift % values.shape[axis]
    return values if shift == 0 else pltpu.roll(values, shift, axis)


def kernel(
    count,
    rows,
    head_hbm,
    ks_hbm,
    class_hbm,
    alpha_hbm,
    shape_hbm,
    bed_hbm,
    code_hbm,
    soil_hbm,
    cover_hbm,
    pond_hbm,
    convey_hbm,
    erod_hbm,
    head_out,
    bed_out,
    head_in,
    ks_in,
    class_in,
    alpha_t,
    shape_t,
    bed_in,
    code_in,
    soil_in,
    cover_in,
    pond_in,
    convey_t,
    erod_t,
    load_sem,
    head_a,
    head_b,
    k_a,
    k_b,
    gain,
    ks,
    alpha,
    shape,
    half_m,
    top_k,
    top_soil,
    falls,
    maps_y,
    levels,
    level_out,
    level_in,
    depths,
    roots,
    maps,
    class_out,
    class_halo,
    class_top,
    tops,
    rest,
    flux_out,
    flux,
    edge,
    edges,
    halo_change,
    packed,
    gathered,
    final_src,
    final_dst,
    fields_y,
    send_sem,
    recv_sem,
    spread_send,
    spread_recv,
    final_send,
    final_recv,
):
    layers = head_hbm.shape[0] // rows
    columns = head_hbm.shape[1]
    strip = bed_in.shape[0]
    width = bed_in.shape[1]
    per = LANES // strip
    groups = columns // LANES
    tiles = layers // TOP
    me = lax.axis_index("tile")
    half = rows // 2
    whole_part = slice(0, layers)
    top_part = slice(0, TOP)
    rest_part = slice(TOP, layers)

    def at(tile):
        return {"tile": tile}

    def peer_of(away):
        return jnp.where(me + away >= count, me + away - count, me + away)

    def exists(side):
        other = me + 2 * side - 1
        return jnp.logical_and(other >= 0, other < count)

    def copy_to(kind, slot, side, src, dst):
        return pltpu.make_async_remote_copy(
            src_ref=src,
            dst_ref=dst,
            send_sem=send_sem.at[kind, slot, side],
            recv_sem=recv_sem.at[kind, slot, 1 - side],
            device_id=at(me + 2 * side - 1),
            device_id_type=pl.DeviceIdType.MESH,
        )

    def push(kind, slot, side, src, dst):
        copy_to(kind, slot, side, src, dst).start()

    def got(kind, slot, side, ref):
        copy_to(kind, slot, 1 - side, ref, ref).wait_recv()

    def sent(kind, slot, side, ref):
        copy_to(kind, slot, side, ref, ref).wait_send()

    maps_y[...] = jnp.zeros_like(maps_y)
    barrier = pltpu.get_barrier_semaphore()
    for away in range(1, count):
        pl.semaphore_signal(
            barrier,
            inc=1,
            device_id=at(peer_of(away)),
            device_id_type=pl.DeviceIdType.MESH,
        )

    loads = [
        pltpu.make_async_copy(
            source.at[:, group * LANES : (group + 1) * LANES],
            target.at[group],
            load_sem.at[index, group],
        )
        for index, (source, target) in enumerate(
            ((head_hbm, head_in), (class_hbm, class_in), (ks_hbm, ks_in))
        )
        for group in range(groups)
    ]
    wide_loads = len(loads)
    loads += [
        pltpu.make_async_copy(source, target, load_sem.at[3, index])
        for index, (source, target) in enumerate(
            (
                (alpha_hbm, alpha_t),
                (shape_hbm, shape_t),
                (cover_hbm, cover_in),
                (pond_hbm, pond_in),
                (soil_hbm, soil_in),
                (code_hbm, code_in),
                (bed_hbm, bed_in),
                (convey_hbm, convey_t),
                (erod_hbm, erod_t),
            )
        )
    ]
    for load in loads:
        load.start()

    falls[:, :, 0:TOP] = jnp.zeros((rows + 2, groups, TOP, LANES), jnp.float32)
    levels[...] = jnp.zeros_like(levels)
    depths[...] = jnp.zeros_like(depths)
    edge[...] = jnp.zeros_like(edge)
    edges[...] = jnp.zeros_like(edges)
    halo_change[...] = jnp.zeros_like(halo_change)

    def soil(found):
        scale = lax.log2(table_pick(found, lambda i: alpha_t[i], alpha_t.shape[0]))
        bend = table_pick(found, lambda i: shape_t[i], shape_t.shape[0])
        return scale, bend, 0.5 / bend - 0.5

    def soil_tile(row, spot, found):
        alpha[row, :, spot], shape[row, :, spot], half_m[row, :, spot] = soil(found)

    def conduct(head, scale, bend, power, full_k):
        log_a = lax.log2(jnp.maximum(-head, TINY)) + scale
        log_p = bend * log_a
        log_w = lax.log2(1.0 + lax.exp2(log_p))
        root = lax.exp2(power * log_w)
        full = root * root
        inner = 1.0 - lax.exp2(log_p - log_a) * full
        return full_k * root * (inner * inner), full

    def tile_spots(part):
        return [slice(t, t + TOP) for t in range(part.start, part.stop, TOP)]

    def conduct_row(head, k_ref, row, part, gains=True):
        for spot in tile_spots(part):
            k, full = conduct(
                head[row, :, spot],
                alpha[row, :, spot],
                shape[row, :, spot],
                half_m[row, :, spot],
                ks[row, :, spot],
            )
            k_ref[row, :, spot] = k
            if gains:
                gain[row, :, spot] = 1.0 / (GAIN_BASE - GAIN_SLOPE * full)

    block_shape = (groups, TOP, LANES)
    low_edge = lax.broadcasted_iota(jnp.int32, block_shape, 1) == TOP - 1
    first_lane = lax.broadcasted_iota(jnp.int32, block_shape, 2) == 0
    last_lane = lax.broadcasted_iota(jnp.int32, block_shape, 2) == LANES - 1

    def from_right(values):
        moved = pltpu.roll(values, LANES - 1, 2)
        return jnp.where(last_lane, jnp.concatenate([moved[1:], moved[:1]], axis=0), moved)

    def from_left(values):
        moved = pltpu.roll(values, 1, 2)
        return jnp.where(first_lane, jnp.concatenate([moved[-1:], moved[:-1]], axis=0), moved)

    def side_flow(h, k):
        right = (k + from_right(k)) * (from_right(h) - h)
        shut = jnp.where(last_lane[:1], 0.0, right[-1:])
        right = jnp.concatenate([right[:-1], shut], axis=0)
        return right - from_left(right)

    def face(src, k_ref, row, other, spot):
        return (k_ref[row, :, spot] + k_ref[other, :, spot]) * (
            src[other, :, spot] - src[row, :, spot]
        )

    def flow_rows(src, dst, k_ref, chain, inward, enter, part=whole_part):
        for spot in tile_spots(part):
            entering = enter(spot)
            for row in chain:
                h, k = src[row, :, spot], k_ref[row, :, spot]
                onward = face(src, k_ref, row, row + inward, spot)
                if spot.stop < layers:
                    lower = slice(spot.start + 1, spot.stop + 1)
                    fall = (k + k_ref[row, :, lower]) * (src[row, :, lower] - h - 1.0)
                else:
                    fall = (k + pltpu.roll(k, TOP - 1, 1)) * (pltpu.roll(h, TOP - 1, 1) - h - 1.0)
                    fall = jnp.where(low_edge, -2.0 * k, fall)
                falls[row, :, spot.start + TOP : spot.stop + TOP] = fall
                fell = falls[row, :, spot.start + TOP - 1 : spot.stop + TOP - 1]
                flow = onward + entering + side_flow(h, k) + (fall - fell)
                entering = -onward
                result = h + flow * gain[row, :, spot]
                if dst is None:
                    return result[:, 0:1]
                dst[row, :, spot] = result

    def strided(ref, row, tile):
        spot = pl.ds(tile * TOP * rows + row, TOP, stride=rows)
        return jnp.stack([ref[group, spot, :] for group in range(groups)])

    def bring(row):
        for tile, spot in enumerate(tile_spots(whole_part)):
            head_a[row + 1, :, spot] = strided(head_in, row, tile)
            ks[row + 1, :, spot] = 0.5 * strided(ks_in, row, tile)

    def bring_soil(row):
        for tile, spot in enumerate(tile_spots(whole_part)):
            soil_tile(row + 1, spot, strided(class_in, row, tile))

    def store_out(row, wanted):
        for tile in wanted:
            for group in range(groups):
                start = (tile * TOP * groups + group) * rows + row
                head_out[pl.ds(start, TOP, stride=groups * rows), :] = head_a[
                    row + 1, group, tile * TOP : (tile + 1) * TOP
                ]

    edge_rows = (0, 1, rows - 2, rows - 1)
    for load in loads[:wide_loads]:
        load.wait()
    for place, row in enumerate(edge_rows):
        bring(row)
        for tile in range(tiles):
            class_out[place, :, tile * TOP : (tile + 1) * TOP] = strided(class_in, row, tile)

    pl.semaphore_wait(barrier, count - 1)

    far = lax.rem(me, 2)

    def both_sides(work, leading):
        for first in range(2):

            @pl.when(leading == first)
            def _():
                work(first)
                work(1 - first)

    def edge_of(side):
        return 1 + side * (rows - 1), 1 - 2 * side

    def face_flux(side, part):
        own, step = edge_of(side)
        conduct_row(head_a, k_a, own, part)
        conduct_row(head_a, k_a, own + step, part)
        for spot in tile_spots(part):
            flux_out[side, :, spot] = face(head_a, k_a, own, own + step, spot)

    def start_side(side):
        there = 1 - side
        own_row, inward = edge_of(side)
        far_row = (rows + 1) * there

        @pl.when(exists(side))
        def _():
            push(HEAD, 0, side, head_a.at[own_row], head_a.at[far_row])
            push(SOIL_C, 0, side, class_out.at[3 * side], class_halo.at[there])
            push(SOIL_K, 0, side, ks.at[own_row], ks.at[far_row])

    both_sides(start_side, far)

    for load in loads[wide_loads : wide_loads + 2]:
        load.wait()
    for row in edge_rows:
        bring_soil(row)

    def start_flux(side):
        there = 1 - side
        own_row, inward = edge_of(side)
        face_flux(side, whole_part)

        @pl.when(exists(side))
        def _():
            push(FLUX, 0, side, flux_out.at[side], flux.at[0, there])
            push(TOP_C, 0, side, class_out.at[1 + side, :, top_part], class_top.at[there])
            push(TOP_K, 0, side, ks.at[own_row + inward, :, top_part], top_k.at[0, there])

    both_sides(start_flux, far)

    for load in loads[wide_loads + 2 :]:
        load.wait()
    coef_y = table_pick(cover_in[...], lambda i: convey_t[i], convey_t.shape[0]) * (
        1.0 - pond_in[...].astype(jnp.float32)
    )
    erode_y = table_pick(soil_in[...], lambda i: erod_t[i], erod_t.shape[0])
    code_y = code_in[...].astype(jnp.float32)
    stacked = jnp.concatenate([coef_y, erode_y, code_y, bed_in[...]], axis=0)
    strip_part = slice(TOP, TOP + strip)
    for kind, field in enumerate((coef_y, erode_y, code_y)):
        maps_y[kind, strip_part] = field
    quads = rows // EDGE
    packed[0] = jnp.zeros((EDGE, LANES), jnp.float32)
    packed[width // EDGE + 1] = jnp.zeros((EDGE, LANES), jnp.float32)
    for block in range(width // LANES):
        upright = jnp.transpose(stacked[:, block * LANES : (block + 1) * LANES])
        for quad in range(LANES // EDGE):
            packed[1 + block * (LANES // EDGE) + quad] = upright[quad * EDGE : (quad + 1) * EDGE]

    def spread(away):
        peer = peer_of(away)
        return pltpu.make_async_remote_copy(
            src_ref=packed.at[pl.ds(peer * quads, quads + 2)],
            dst_ref=gathered.at[me],
            send_sem=spread_send.at[away],
            recv_sem=spread_recv.at[away],
            device_id=at(peer),
            device_id_type=pl.DeviceIdType.MESH,
        )

    by_distance = sorted(range(1, count), key=lambda away: abs(2 * away - count))
    for away in by_distance:
        spread(away).start()
    gathered[me] = packed[pl.ds(me * quads, quads + 2)]

    ends = (slice(TOP, 2 * TOP), slice(strip, strip + TOP))
    beyond = (slice(0, TOP), slice(strip + TOP, strip + 2 * TOP))
    for side in range(2):

        @pl.when(exists(side))
        def _():
            push(MAPS, 0, side, maps_y.at[:, ends[side]], maps_y.at[:, beyond[1 - side]])

    own = slice(EDGE, EDGE + rows)
    piece = lax.broadcasted_iota(jnp.int32, (rows + 2 * EDGE, LANES), 1) // strip

    def assemble():
        for away in range(1, count):
            spread(away).wait()
        for group in range(groups):
            blocks = [
                jnp.concatenate([gathered[group * per + part, q] for q in range(quads + 2)], axis=0)
                for part in range(per)
            ]
            for kind in range(4):
                joined = None
                for part in range(per):
                    block = turn(blocks[part], (part - kind) * strip, 1)
                    joined = block if joined is None else jnp.where(piece == part, block, joined)
                spot = slice(group * LANES, (group + 1) * LANES)
                if kind < 3:
                    maps[kind, :, spot] = joined
                else:
                    levels[0, :, spot] = joined

    def shifted(values, first, second):
        lane = lax.broadcasted_iota(jnp.int32, values.shape, 1)
        values = turn(values, -second, 1)
        if second == 1:
            values = jnp.where(lane == values.shape[1] - 1, 0.0, values)
        if second == -1:
            values = jnp.where(lane == 0, 0.0, values)
        return turn(values, -first, 0)

    def slope_root(code, level, shifts):
        target = jnp.zeros_like(level)
        scale = jnp.ones_like(level)
        for course, (first, second) in enumerate(shifts):
            chosen = code == course
            target = jnp.where(chosen, shifted(level, first, second), target)
            if first * second != 0:
                scale = jnp.where(chosen, 1.0 / math.sqrt(2.0), scale)
        slope = MIN_SLOPE + jnp.maximum(level - target, 0.0) * scale
        return jnp.sqrt(slope)

    def surface(fields, root, depth, shifts):
        coef, erode, code = fields
        power = lax.exp2((2.0 / 3.0) * lax.log2(jnp.maximum(depth, TINY)))
        drive = coef * root * power
        outflow = depth * drive / (1.0 + drive)
        sediment = erode * outflow * root

        def balance(field):
            total = -field
            for course, (first, second) in enumerate(shifts):
                passed = jnp.where(code == course, field, 0.0)
                total = total + shifted(passed, -first, -second)
            return total

        return outflow, sediment, balance

    shifts_x = tuple(zip(SHIFT_X, SHIFT_Y))
    shifts_y = tuple(zip(SHIFT_Y, SHIFT_X))
    lead = (LANES - strip) // 2

    def finish(kind, away):
        peer = peer_of(away)
        return pltpu.make_async_remote_copy(
            src_ref=final_src.at[kind, peer],
            dst_ref=final_dst.at[kind, me],
            send_sem=final_send.at[kind, away],
            recv_sem=final_recv.at[kind, away],
            device_id=at(peer),
            device_id_type=pl.DeviceIdType.MESH,
        )

    def hand_out(kind, field):
        for part in range(per):
            window = turn(field, lead - strip * part, 1)
            for group in range(groups):
                final_src[kind, group * per + part] = window[:, group * LANES : (group + 1) * LANES]
        for away in by_distance:
            finish(kind, away).start()
        final_dst[kind, me] = final_src[kind, me]

    def collect(kind):
        for away in range(1, count):
            finish(kind, away).wait()
        members = LANES // rows
        for block in range(width // LANES):
            part = final_dst[kind, block * members : (block + 1) * members]
            seen = jnp.transpose(part.reshape(LANES, LANES))[lead - TOP : lead + strip + TOP]
            line = lax.broadcasted_iota(jnp.int32, seen.shape, 0) + (me * strip - TOP)
            inside = jnp.logical_and(line >= 0, line < strip * count)
            fields_y[kind, :, block * LANES : (block + 1) * LANES] = jnp.where(inside, seen, 0.0)

    for row in range(2, rows - 2):
        bring(row)
        bring_soil(row)
        conduct_row(head_a, k_a, row + 1, rest_part)

    def put_row(ref, row, values):
        for group in range(groups):
            ref[row : row + 1, group * LANES : (group + 1) * LANES] = values[group]

    def add_row(ref, values):
        for group in range(groups):
            ref[group, 0:1] = ref[group, 0:1] + values[:, group * LANES : (group + 1) * LANES]

    @pl.loop(0, STEPS)
    def _(step):
        slot = lax.rem(step, 2)
        other = 1 - slot
        going = step < STEPS - 1

        for row in range(1, rows + 1):
            conduct_row(head_a, k_a, row, top_part)

        def side_work(side):
            there = 1 - side
            own_row, inward = edge_of(side)
            halo = own_row - inward
            here = exists(side)
            outer = jnp.where(here, halo, own_row)
            second = own_row + inward
            third = second + inward

            flow_rows(
                head_a,
                head_b,
                k_a,
                [own_row + ahead * inward for ahead in range(1, half)],
                inward,
                lambda spot: face(head_a, k_a, second, own_row, spot),
            )
            conduct_row(head_b, k_b, second, whole_part)
            conduct_row(head_b, k_b, third, whole_part)
            conduct_row(head_b, k_b, third + inward, top_part)

            @pl.when(jnp.logical_and(here, step == 0))
            def _():
                got(SOIL_C, 0, side, class_halo.at[side])
                got(SOIL_K, 0, side, ks.at[halo])
                sent(SOIL_C, 0, side, class_halo.at[side])
                sent(SOIL_K, 0, side, ks.at[halo])
                sent(HEAD, 0, side, head_a.at[halo])
                for spot in tile_spots(whole_part):
                    soil_tile(halo, spot, class_halo[side, :, spot])
                got(HEAD, 0, side, head_a.at[halo])

            @pl.when(jnp.logical_and(here, step == 1))
            def _():
                got(TOP_C, 0, side, class_top.at[side])
                got(TOP_K, 0, side, top_k.at[0, side])
                sent(TOP_C, 0, side, class_top.at[side])
                sent(TOP_K, 0, side, top_k.at[0, side])
                a, b, c = soil(class_top[side])
                top_soil[0, side], top_soil[1, side], top_soil[2, side] = a, b, c

            @pl.when(jnp.logical_and(here, step > 0))
            def _():
                got(TOPS, slot, side, tops.at[slot, side])
                got(REST, slot, side, rest.at[slot, side])
                sent(REST, slot, side, rest.at[slot, side])
                head_a[halo, :, top_part] = tops[slot, side, there]
                head_a[halo, :, rest_part] = rest[slot, side]
                add_row(head_a.at[halo], halo_change[side, 0:1])
                beyond = tops.at[slot, side, side]
                add_row(beyond, halo_change[side, 1:2])
                top_k[1, side], _unused = conduct(
                    beyond[...],
                    top_soil[0, side],
                    top_soil[1, side],
                    top_soil[2, side],
                    top_k[0, side],
                )

            conduct_row(head_a, k_a, halo, whole_part)
            flow_rows(
                head_a,
                head_b,
                k_a,
                [own_row],
                inward,
                lambda spot: face(head_a, k_a, own_row, outer, spot),
            )
            conduct_row(head_b, k_b, own_row, whole_part)
            flow_rows(
                head_b,
                head_a,
                k_b,
                [second],
                inward,
                lambda spot: face(head_b, k_b, second, own_row, spot),
            )
            third_top = flow_rows(
                head_b,
                None,
                k_b,
                [third],
                inward,
                lambda spot: face(head_b, k_b, third, second, spot),
                part=top_part,
            )
            put_row(edge.at[side], 2, jnp.maximum(third_top, 0.0))
            put_row(edge.at[side], 1, jnp.maximum(head_a[second, :, 0:1], 0.0))

            @pl.when(jnp.logical_and(here, step == 0))
            def _():
                got(FLUX, 0, side, flux.at[0, side])
                sent(FLUX, 0, side, flux.at[0, side])

            @pl.when(jnp.logical_and(here, step > 0))
            def _():
                flux[slot, side, :, top_part] = (k_a[halo, :, top_part] + top_k[1, side]) * (
                    tops[slot, side, side] - head_a[halo, :, top_part]
                )
                got(FLUX, slot, side, flux.at[slot, side, :, rest_part])
                sent(FLUX, slot, side, flux.at[slot, side, :, rest_part])

            flow_rows(
                head_a, head_b, k_a, [halo], inward, lambda spot: flux[slot, side, :, spot]
            )
            conduct_row(head_b, k_b, halo, whole_part, gains=False)
            flow_rows(
                head_b,
                head_a,
                k_b,
                [own_row],
                inward,
                lambda spot: face(head_b, k_b, own_row, outer, spot),
            )
            put_row(edge.at[side], 0, jnp.maximum(head_a[own_row, :, 0:1], 0.0))

            @pl.when(here)
            def _():
                push(DEPTH, other, side, edge.at[side], edges.at[other, there])

            @pl.when(jnp.logical_and(here, going))
            def _():
                low = 1 + side * (rows - 2)
                push(
                    TOPS, other, side, head_a.at[pl.ds(low, 2), :, top_part], tops.at[other, there]
                )
                push(REST, other, side, head_a.at[own_row, :, rest_part], rest.at[other, there])

            @pl.when(going)
            def _():
                face_flux(side, rest_part)

            @pl.when(jnp.logical_and(here, going))
            def _():
                push(
                    FLUX,
                    other,
                    side,
                    flux_out.at[side, :, rest_part],
                    flux.at[other, there, :, rest_part],
                )

        both_sides(side_work, jnp.where(going, far, 1 - far))

        for row in (half, half + 1):
            conduct_row(head_b, k_b, row, rest_part)
        flow_rows(
            head_b,
            head_a,
            k_b,
            range(3, rows - 1),
            1,
            lambda spot: face(head_b, k_b, 3, 2, spot),
        )

        @pl.when(going)
        def _():
            for row in range(3, rows - 1):
                conduct_row(head_a, k_a, row, rest_part)

        @pl.when(step == 0)
        def _():
            assemble()

        for row in range(rows):
            put_row(depths, EDGE + row, jnp.maximum(head_a[row + 1, :, 0:1], 0.0))

        @pl.when(step == STEPS - 1)
        def _():
            hand_out(0, depths[own])
            for row in range(rows):
                store_out(row, range(1, tiles))

        for side in range(2):

            @pl.when(jnp.logical_and(exists(side), step > 0))
            def _():
                got(LEVEL, slot, side, level_in.at[slot, side])
                sent(LEVEL, slot, side, level_in.at[slot, side])
                beside = side * (rows + EDGE)
                levels[slot, beside : beside + EDGE] = level_in[slot, side]

        roots[...] = slope_root(maps[2], levels[slot], shifts_x)

        for side in range(2):

            @pl.when(exists(side))
            def _():
                got(DEPTH, other, side, edges.at[other, side])
                sent(DEPTH, other, side, edges.at[other, side])

        for away in range(3):
            spot = EDGE - 1 - away
            depths[spot : spot + 1] = edges[other, 0, away : away + 1]
            spot = EDGE + rows + away
            depths[spot : spot + 1] = edges[other, 1, away : away + 1]

        outflow, sediment, balance = surface(
            (maps[0], maps[1], maps[2]), roots[...], depths[...], shifts_x
        )
        change = balance(outflow)

        for side in range(2):

            @pl.when(jnp.logical_and(exists(side), going))
            def _():
                sent(TOPS, other, side, tops.at[other, side])

        for row in range(rows):
            spot = EDGE + row
            add_row(head_a.at[row + 1], change[spot : spot + 1])
        for away in range(2):
            spot = EDGE - 1 - away
            halo_change[0, away : away + 1] = change[spot : spot + 1]
            spot = EDGE + rows + away
            halo_change[1, away : away + 1] = change[spot : spot + 1]

        @pl.when(going)
        def _():
            fresh = levels[slot, own] + BED_RATE * balance(sediment)[own]
            levels[other, own] = fresh
            level_out[other, 0] = fresh[0:EDGE]
            level_out[other, 1] = fresh[rows - EDGE : rows]

        for side in range(2):

            @pl.when(jnp.logical_and(exists(side), going))
            def _():
                push(LEVEL, other, side, level_out.at[other, side], level_in.at[other, 1 - side])

        @pl.when(step == STEPS - 2)
        def _():
            hand_out(1, levels[other, own])


    for row in range(rows):
        store_out(row, range(1))
    for side in range(2):

        @pl.when(exists(side))
        def _():
            got(MAPS, 0, side, maps_y.at[:, beyond[side]])
            sent(MAPS, 0, side, maps_y.at[:, beyond[side]])

    collect(1)
    root_y = slope_root(maps_y[2], fields_y[1], shifts_y)
    collect(0)
    _unused, sediment, balance = surface(
        (maps_y[0], maps_y[1], maps_y[2]), root_y, fields_y[0], shifts_y
    )
    bed_out[...] = fields_y[1, strip_part] + BED_RATE * balance(sediment)[strip_part]


def on_device(
    pressure,
    conductivity,
    soil_class,
    vg_alpha,
    vg_shape,
    bed,
    flow_code,
    surface_soil,
    cover_class,
    ponding,
    conveyance,
    erodibility,
):
    count = lax.axis_size("tile")
    layers, rows, columns = pressure.shape
    strip, width = bed.shape
    groups = columns // LANES
    head = pressure.reshape(layers * rows, columns)
    ks = conductivity.reshape(layers * rows, columns)
    classes = soil_class.reshape(layers * rows, columns)
    vmem = pl.BlockSpec(memory_space=pltpu.VMEM)
    hbm = pl.BlockSpec(memory_space=pltpu.HBM)
    pin = lambda x: pltpu.with_memory_space_constraint(x, pltpu.HBM)
    wide = pltpu.VMEM((rows + 2, groups, layers, LANES), jnp.float32)
    dma = pltpu.SemaphoreType.DMA
    head_out, bed_out = pl.pallas_call(
        functools.partial(kernel, count, rows),
        out_shape=(
            jax.ShapeDtypeStruct((layers * rows * groups, LANES), jnp.float32),
            jax.ShapeDtypeStruct((strip, width), jnp.float32),
        ),
        in_specs=[hbm] * 12,
        out_specs=(vmem, vmem),
        scratch_shapes=[
            pltpu.VMEM((groups, layers * rows, LANES), jnp.float32),
            pltpu.VMEM((groups, layers * rows, LANES), jnp.float32),
            pltpu.VMEM((groups, layers * rows, LANES), jnp.int32),
            pltpu.SMEM(vg_alpha.shape, jnp.float32),
            pltpu.SMEM(vg_shape.shape, jnp.float32),
            pltpu.VMEM(bed.shape, jnp.float32),
            pltpu.VMEM(bed.shape, jnp.int32),
            pltpu.VMEM(bed.shape, jnp.int32),
            pltpu.VMEM(bed.shape, jnp.int32),
            pltpu.VMEM(bed.shape, jnp.int32),
            pltpu.SMEM(conveyance.shape, jnp.float32),
            pltpu.SMEM(erodibility.shape, jnp.float32),
            dma((4, max(groups, 9))),
            wide,
            wide,
            wide,
            wide,
            wide,
            wide,
            wide,
            wide,
            wide,
            pltpu.VMEM((2, 2, groups, TOP, LANES), jnp.float32),
            pltpu.VMEM((3, 2, groups, TOP, LANES), jnp.float32),
            pltpu.VMEM((rows + 2, groups, layers + TOP, LANES), jnp.float32),
            pltpu.VMEM((3, strip + 2 * TOP, width), jnp.float32),
            pltpu.VMEM((2, rows + 2 * EDGE, columns), jnp.float32),
            pltpu.VMEM((2, 2, EDGE, columns), jnp.float32),
            pltpu.VMEM((2, 2, EDGE, columns), jnp.float32),
            pltpu.VMEM((rows + 2 * EDGE, columns), jnp.float32),
            pltpu.VMEM((rows + 2 * EDGE, columns), jnp.float32),
            pltpu.VMEM((3, rows + 2 * EDGE, columns), jnp.float32),
            pltpu.VMEM((4, groups, layers, LANES), jnp.int32),
            pltpu.VMEM((2, groups, layers, LANES), jnp.int32),
            pltpu.VMEM((2, groups, TOP, LANES), jnp.int32),
            pltpu.VMEM((2, 2, 2, groups, TOP, LANES), jnp.float32),
            pltpu.VMEM((2, 2, groups, layers - TOP, LANES), jnp.float32),
            pltpu.VMEM((2, groups, layers, LANES), jnp.float32),
            pltpu.VMEM((2, 2, groups, layers, LANES), jnp.float32),
            pltpu.VMEM((2, EDGE, columns), jnp.float32),
            pltpu.VMEM((2, 2, EDGE, columns), jnp.float32),
            pltpu.VMEM((2, EDGE, columns), jnp.float32),
            pltpu.VMEM((width // EDGE + 2, EDGE, LANES), jnp.float32),
            pltpu.VMEM((count, rows // EDGE + 2, EDGE, LANES), jnp.float32),
            pltpu.VMEM((2, count, rows, LANES), jnp.float32),
            pltpu.VMEM((2, count, rows, LANES), jnp.float32),
            pltpu.VMEM((2, strip + 2 * TOP, width), jnp.float32),
            dma((KINDS, 2, 2)),
            dma((KINDS, 2, 2)),
            dma((count,)),
            dma((count,)),
            dma((2, count)),
            dma((2, count)),
        ],
        compiler_params=pltpu.CompilerParams(
            collective_id=0, has_side_effects=True, vmem_limit_bytes=40 * 1024 * 1024
        ),
    )(
        pin(head),
        pin(ks),
        pin(classes),
        pin(vg_alpha),
        pin(vg_shape),
        pin(bed),
        pin(flow_code),
        pin(surface_soil),
        pin(cover_class),
        pin(ponding),
        pin(conveyance),
        pin(erodibility),
    )
    head_out = jnp.swapaxes(head_out.reshape(layers, groups, rows, LANES), 1, 2)
    return head_out.reshape(layers, rows, columns), bed_out


def solution(mesh):
    in_specs = (
        P("member", "tile", None),
        P("member", "tile", None),
        P("member", "tile", None),
        P(),
        P(),
        P("tile", "member"),
        P("tile", "member"),
        P("tile", "member"),
        P("tile", "member"),
        P("tile", "member"),
        P(),
        P(),
    )
    out_specs = (P("member", "tile", None), P("tile", "member"))
    return jax.shard_map(
        on_device, mesh=mesh, in_specs=in_specs, out_specs=out_specs, check_vma=False
    )
```

```python
import functools
import math

import jax
import jax.numpy as jnp
from jax import lax
from jax.experimental import pallas as pl
from jax.experimental.pallas import tpu as pltpu
from jax.sharding import PartitionSpec as P

STEPS = 4
RELAX_STEP = 0.08
CAPACITY = 2.0
GAIN_BASE = (1.0 + CAPACITY) / RELAX_STEP
GAIN_SLOPE = CAPACITY / RELAX_STEP
MIN_SLOPE = 0.01
BED_RATE = 2.0
SHIFT_X = (1, 1, 0, -1, -1, -1, 0, 1)
SHIFT_Y = (0, 1, 1, 1, 0, -1, -1, -1)
TINY = 1.2e-38
LANES = 128
KINDS = 11
TOPS, REST, FLUX, LEVEL, DEPTH, HEAD, SOIL_K, SOIL_C, TOP_K, TOP_C, MAPS = range(KINDS)
HALO = 2
TOP = 8
EDGE = 4


def table_pick(classes, table, entries):
    picked = jnp.full(classes.shape, table(0), jnp.float32)
    for entry in range(1, entries):
        picked = jnp.where(classes == entry, table(entry), picked)
    return picked


def turn(values, shift, axis):
    shift = shift % values.shape[axis]
    return values if shift == 0 else pltpu.roll(values, shift, axis)


def kernel(
    count,
    rows,
    head_hbm,
    ks_hbm,
    class_hbm,
    alpha_hbm,
    shape_hbm,
    bed_hbm,
    code_hbm,
    soil_hbm,
    cover_hbm,
    pond_hbm,
    convey_hbm,
    erod_hbm,
    head_out,
    bed_out,
    head_in,
    ks_in,
    class_in,
    alpha_t,
    shape_t,
    bed_in,
    code_in,
    soil_in,
    cover_in,
    pond_in,
    convey_t,
    erod_t,
    load_sem,
    head_a,
    head_b,
    k_a,
    k_b,
    gain,
    ks,
    alpha,
    shape,
    half_m,
    top_k,
    top_soil,
    falls,
    maps_y,
    levels,
    level_out,
    level_in,
    depths,
    roots,
    maps,
    class_out,
    class_halo,
    class_top,
    tops,
    rest,
    flux_out,
    flux,
    edge,
    edges,
    halo_change,
    packed,
    gathered,
    final_src,
    final_dst,
    fields_y,
    send_sem,
    recv_sem,
    spread_send,
    spread_recv,
    final_send,
    final_recv,
):
    layers = head_hbm.shape[0] // rows
    columns = head_hbm.shape[1]
    strip = bed_in.shape[0]
    width = bed_in.shape[1]
    per = LANES // strip
    groups = columns // LANES
    tiles = layers // TOP
    me = lax.axis_index("tile")
    half = rows // 2
    whole_part = slice(0, layers)
    top_part = slice(0, TOP)
    rest_part = slice(TOP, layers)

    def at(tile):
        return {"tile": tile}

    def peer_of(away):
        return jnp.where(me + away >= count, me + away - count, me + away)

    def exists(side):
        other = me + 2 * side - 1
        return jnp.logical_and(other >= 0, other < count)

    def copy_to(kind, slot, side, src, dst):
        return pltpu.make_async_remote_copy(
            src_ref=src,
            dst_ref=dst,
            send_sem=send_sem.at[kind, slot, side],
            recv_sem=recv_sem.at[kind, slot, 1 - side],
            device_id=at(me + 2 * side - 1),
            device_id_type=pl.DeviceIdType.MESH,
        )

    def push(kind, slot, side, src, dst):
        copy_to(kind, slot, side, src, dst).start()

    def got(kind, slot, side, ref):
        copy_to(kind, slot, 1 - side, ref, ref).wait_recv()

    def sent(kind, slot, side, ref):
        copy_to(kind, slot, side, ref, ref).wait_send()

    maps_y[...] = jnp.zeros_like(maps_y)
    barrier = pltpu.get_barrier_semaphore()
    for away in range(1, count):
        pl.semaphore_signal(
            barrier,
            inc=1,
            device_id=at(peer_of(away)),
            device_id_type=pl.DeviceIdType.MESH,
        )

    loads = [
        pltpu.make_async_copy(
            source.at[:, group * LANES : (group + 1) * LANES],
            target.at[group],
            load_sem.at[index, group],
        )
        for index, (source, target) in enumerate(
            ((head_hbm, head_in), (class_hbm, class_in), (ks_hbm, ks_in))
        )
        for group in range(groups)
    ]
    wide_loads = len(loads)
    loads += [
        pltpu.make_async_copy(source, target, load_sem.at[3, index])
        for index, (source, target) in enumerate(
            (
                (alpha_hbm, alpha_t),
                (shape_hbm, shape_t),
                (cover_hbm, cover_in),
                (pond_hbm, pond_in),
                (soil_hbm, soil_in),
                (code_hbm, code_in),
                (bed_hbm, bed_in),
                (convey_hbm, convey_t),
                (erod_hbm, erod_t),
            )
        )
    ]
    for load in loads:
        load.start()

    falls[:, :, 0:TOP] = jnp.zeros((rows + 2, groups, TOP, LANES), jnp.float32)
    levels[...] = jnp.zeros_like(levels)
    depths[...] = jnp.zeros_like(depths)
    edge[...] = jnp.zeros_like(edge)
    edges[...] = jnp.zeros_like(edges)
    halo_change[...] = jnp.zeros_like(halo_change)

    def soil(found):
        scale = lax.log2(table_pick(found, lambda i: alpha_t[i], alpha_t.shape[0]))
        bend = table_pick(found, lambda i: shape_t[i], shape_t.shape[0])
        return scale, bend, 0.5 / bend - 0.5

    def soil_tile(row, spot, found):
        alpha[row, :, spot], shape[row, :, spot], half_m[row, :, spot] = soil(found)

    def conduct(head, scale, bend, power, full_k):
        log_a = lax.log2(jnp.maximum(-head, TINY)) + scale
        log_p = bend * log_a
        log_w = lax.log2(1.0 + lax.exp2(log_p))
        root = lax.exp2(power * log_w)
        full = root * root
        inner = 1.0 - lax.exp2(log_p - log_a) * full
        return full_k * root * (inner * inner), full

    def tile_spots(part):
        return [slice(t, t + TOP) for t in range(part.start, part.stop, TOP)]

    def conduct_row(head, k_ref, row, part, gains=True):
        for spot in tile_spots(part):
            k, full = conduct(
                head[row, :, spot],
                alpha[row, :, spot],
                shape[row, :, spot],
                half_m[row, :, spot],
                ks[row, :, spot],
            )
            k_ref[row, :, spot] = k
            if gains:
                gain[row, :, spot] = 1.0 / (GAIN_BASE - GAIN_SLOPE * full)

    block_shape = (groups, TOP, LANES)
    low_edge = lax.broadcasted_iota(jnp.int32, block_shape, 1) == TOP - 1
    first_lane = lax.broadcasted_iota(jnp.int32, block_shape, 2) == 0
    last_lane = lax.broadcasted_iota(jnp.int32, block_shape, 2) == LANES - 1

    def from_right(values):
        moved = pltpu.roll(values, LANES - 1, 2)
        return jnp.where(last_lane, jnp.concatenate([moved[1:], moved[:1]], axis=0), moved)

    def from_left(values):
        moved = pltpu.roll(values, 1, 2)
        return jnp.where(first_lane, jnp.concatenate([moved[-1:], moved[:-1]], axis=0), moved)

    def side_flow(h, k):
        right = (k + from_right(k)) * (from_right(h) - h)
        shut = jnp.where(last_lane[:1], 0.0, right[-1:])
        right = jnp.concatenate([right[:-1], shut], axis=0)
        return right - from_left(right)

    def face(src, k_ref, row, other, spot):
        return (k_ref[row, :, spot] + k_ref[other, :, spot]) * (
            src[other, :, spot] - src[row, :, spot]
        )

    def flow_rows(src, dst, k_ref, chain, inward, enter, part=whole_part):
        for spot in tile_spots(part):
            entering = enter(spot)
            for row in chain:
                h, k = src[row, :, spot], k_ref[row, :, spot]
                onward = face(src, k_ref, row, row + inward, spot)
                if spot.stop < layers:
                    lower = slice(spot.start + 1, spot.stop + 1)
                    fall = (k + k_ref[row, :, lower]) * (src[row, :, lower] - h - 1.0)
                else:
                    fall = (k + pltpu.roll(k, TOP - 1, 1)) * (pltpu.roll(h, TOP - 1, 1) - h - 1.0)
                    fall = jnp.where(low_edge, -2.0 * k, fall)
                falls[row, :, spot.start + TOP : spot.stop + TOP] = fall
                fell = falls[row, :, spot.start + TOP - 1 : spot.stop + TOP - 1]
                flow = onward + entering + side_flow(h, k) + (fall - fell)
                entering = -onward
                result = h + flow * gain[row, :, spot]
                if dst is None:
                    return result[:, 0:1]
                dst[row, :, spot] = result

    def strided(ref, row, tile):
        spot = pl.ds(tile * TOP * rows + row, TOP, stride=rows)
        return jnp.stack([ref[group, spot, :] for group in range(groups)])

    def bring(row):
        for tile, spot in enumerate(tile_spots(whole_part)):
            head_a[row + 1, :, spot] = strided(head_in, row, tile)
            ks[row + 1, :, spot] = 0.5 * strided(ks_in, row, tile)

    def bring_soil(row):
        for tile, spot in enumerate(tile_spots(whole_part)):
            soil_tile(row + 1, spot, strided(class_in, row, tile))

    def store_out(row, wanted):
        for tile in wanted:
            for group in range(groups):
                start = (tile * TOP * groups + group) * rows + row
                head_out[pl.ds(start, TOP, stride=groups * rows), :] = head_a[
                    row + 1, group, tile * TOP : (tile + 1) * TOP
                ]

    edge_rows = (0, 1, rows - 2, rows - 1)

    def bring_edge(place):
        row = edge_rows[place]
        bring(row)
        for tile in range(tiles):
            class_out[place, :, tile * TOP : (tile + 1) * TOP] = strided(class_in, row, tile)

    for load in loads[:wide_loads]:
        load.wait()
    pl.semaphore_wait(barrier, count - 1)

    far = lax.rem(me, 2)

    def both_sides(work, leading):
        for first in range(2):

            @pl.when(leading == first)
            def _():
                work(first, True)
                work(1 - first, False)

    def edge_of(side):
        return 1 + side * (rows - 1), 1 - 2 * side

    def face_flux(side, part):
        own, step = edge_of(side)
        conduct_row(head_a, k_a, own, part)
        conduct_row(head_a, k_a, own + step, part)
        for spot in tile_spots(part):
            flux_out[side, :, spot] = face(head_a, k_a, own, own + step, spot)

    def start_side(side, leads):
        there = 1 - side
        own_row, inward = edge_of(side)
        far_row = (rows + 1) * there
        bring_edge(3 * side)

        @pl.when(exists(side))
        def _():
            push(HEAD, 0, side, head_a.at[own_row, :, top_part], tops.at[0, there, side])
            push(REST, 0, side, head_a.at[own_row, :, rest_part], rest.at[0, there])
            push(SOIL_C, 0, side, class_out.at[3 * side], class_halo.at[there])
            push(SOIL_K, 0, side, ks.at[own_row], ks.at[far_row])

    both_sides(start_side, far)

    for load in loads[wide_loads : wide_loads + 2]:
        load.wait()
    for place in (1, 2):
        bring_edge(place)
    for row in edge_rows:
        bring_soil(row)

    def start_flux(side, leads):
        there = 1 - side
        own_row, inward = edge_of(side)
        face_flux(side, whole_part)

        @pl.when(exists(side))
        def _():
            push(FLUX, 0, side, flux_out.at[side], flux.at[0, there])
            push(TOP_C, 0, side, class_out.at[1 + side, :, top_part], class_top.at[there])
            push(TOP_K, 0, side, ks.at[own_row + inward, :, top_part], top_k.at[0, there])

    both_sides(start_flux, far)

    for load in loads[wide_loads + 2 :]:
        load.wait()
    coef_y = table_pick(cover_in[...], lambda i: convey_t[i], convey_t.shape[0]) * (
        1.0 - pond_in[...].astype(jnp.float32)
    )
    erode_y = table_pick(soil_in[...], lambda i: erod_t[i], erod_t.shape[0])
    code_y = code_in[...].astype(jnp.float32)
    stacked = jnp.concatenate([coef_y, erode_y, code_y, bed_in[...]], axis=0)
    strip_part = slice(TOP, TOP + strip)
    for kind, field in enumerate((coef_y, erode_y, code_y)):
        maps_y[kind, strip_part] = field
    quads = rows // EDGE
    packed[0] = jnp.zeros((EDGE, LANES), jnp.float32)
    packed[width // EDGE + 1] = jnp.zeros((EDGE, LANES), jnp.float32)
    for block in range(width // LANES):
        upright = jnp.transpose(stacked[:, block * LANES : (block + 1) * LANES])
        for quad in range(LANES // EDGE):
            packed[1 + block * (LANES // EDGE) + quad] = upright[quad * EDGE : (quad + 1) * EDGE]

    def spread(away):
        peer = peer_of(away)
        return pltpu.make_async_remote_copy(
            src_ref=packed.at[pl.ds(peer * quads, quads + 2)],
            dst_ref=gathered.at[me],
            send_sem=spread_send.at[away],
            recv_sem=spread_recv.at[away],
            device_id=at(peer),
            device_id_type=pl.DeviceIdType.MESH,
        )

    by_distance = sorted(range(1, count), key=lambda away: abs(2 * away - count))
    for away in by_distance:
        spread(away).start()
    gathered[me] = packed[pl.ds(me * quads, quads + 2)]

    ends = (slice(TOP, 2 * TOP), slice(strip, strip + TOP))
    beyond = (slice(0, TOP), slice(strip + TOP, strip + 2 * TOP))
    for side in range(2):

        @pl.when(exists(side))
        def _():
            push(MAPS, 0, side, maps_y.at[:, ends[side]], maps_y.at[:, beyond[1 - side]])

    own = slice(EDGE, EDGE + rows)
    piece = lax.broadcasted_iota(jnp.int32, (rows + 2 * EDGE, LANES), 1) // strip

    def assemble():
        for away in range(1, count):
            spread(away).wait()
        for group in range(groups):
            blocks = [
                jnp.concatenate([gathered[group * per + part, q] for q in range(quads + 2)], axis=0)
                for part in range(per)
            ]
            for kind in range(4):
                joined = None
                for part in range(per):
                    block = turn(blocks[part], (part - kind) * strip, 1)
                    joined = block if joined is None else jnp.where(piece == part, block, joined)
                spot = slice(group * LANES, (group + 1) * LANES)
                if kind < 3:
                    maps[kind, :, spot] = joined
                else:
                    levels[0, :, spot] = joined

    def shifted(values, first, second):
        lane = lax.broadcasted_iota(jnp.int32, values.shape, 1)
        values = turn(values, -second, 1)
        if second == 1:
            values = jnp.where(lane == values.shape[1] - 1, 0.0, values)
        if second == -1:
            values = jnp.where(lane == 0, 0.0, values)
        return turn(values, -first, 0)

    def slope_root(code, level, shifts):
        target = jnp.zeros_like(level)
        scale = jnp.ones_like(level)
        for course, (first, second) in enumerate(shifts):
            chosen = code == course
            target = jnp.where(chosen, shifted(level, first, second), target)
            if first * second != 0:
                scale = jnp.where(chosen, 1.0 / math.sqrt(2.0), scale)
        slope = MIN_SLOPE + jnp.maximum(level - target, 0.0) * scale
        return jnp.sqrt(slope)

    def surface(fields, root, depth, shifts):
        coef, erode, code = fields
        power = lax.exp2((2.0 / 3.0) * lax.log2(jnp.maximum(depth, TINY)))
        drive = coef * root * power
        outflow = depth * drive / (1.0 + drive)
        sediment = erode * outflow * root

        def balance(field):
            total = -field
            for course, (first, second) in enumerate(shifts):
                passed = jnp.where(code == course, field, 0.0)
                total = total + shifted(passed, -first, -second)
            return total

        return outflow, sediment, balance

    shifts_x = tuple(zip(SHIFT_X, SHIFT_Y))
    shifts_y = tuple(zip(SHIFT_Y, SHIFT_X))
    lead = (LANES - strip) // 2

    def finish(kind, away):
        peer = peer_of(away)
        return pltpu.make_async_remote_copy(
            src_ref=final_src.at[kind, peer],
            dst_ref=final_dst.at[kind, me],
            send_sem=final_send.at[kind, away],
            recv_sem=final_recv.at[kind, away],
            device_id=at(peer),
            device_id_type=pl.DeviceIdType.MESH,
        )

    def hand_out(kind, field):
        for part in range(per):
            window = turn(field, lead - strip * part, 1)
            for group in range(groups):
                final_src[kind, group * per + part] = window[:, group * LANES : (group + 1) * LANES]
        for away in by_distance:
            finish(kind, away).start()
        final_dst[kind, me] = final_src[kind, me]

    def collect(kind):
        for away in range(1, count):
            finish(kind, away).wait()
        members = LANES // rows
        for block in range(width // LANES):
            part = final_dst[kind, block * members : (block + 1) * members]
            seen = jnp.transpose(part.reshape(LANES, LANES))[lead - TOP : lead + strip + TOP]
            line = lax.broadcasted_iota(jnp.int32, seen.shape, 0) + (me * strip - TOP)
            inside = jnp.logical_and(line >= 0, line < strip * count)
            fields_y[kind, :, block * LANES : (block + 1) * LANES] = jnp.where(inside, seen, 0.0)

    for row in range(2, rows - 2):
        bring(row)
        bring_soil(row)
        conduct_row(head_a, k_a, row + 1, rest_part)

    def put_row(ref, row, values):
        for group in range(groups):
            ref[row : row + 1, group * LANES : (group + 1) * LANES] = values[group]

    def add_row(ref, values):
        for group in range(groups):
            ref[group, 0:1] = ref[group, 0:1] + values[:, group * LANES : (group + 1) * LANES]

    @pl.loop(0, STEPS)
    def _(step):
        slot = lax.rem(step, 2)
        other = 1 - slot
        going = step < STEPS - 1

        def side_work(side, leads):
            there = 1 - side
            own_row, inward = edge_of(side)
            halo = own_row - inward
            here = exists(side)
            outer = jnp.where(here, halo, own_row)
            second = own_row + inward
            third = second + inward
            for ahead in range(half + 1 if leads else half - 1):
                conduct_row(head_a, k_a, own_row + ahead * inward, top_part)

            flow_rows(
                head_a,
                head_b,
                k_a,
                [own_row + ahead * inward for ahead in range(1, half)],
                inward,
                lambda spot: face(head_a, k_a, second, own_row, spot),
            )
            conduct_row(head_b, k_b, second, whole_part)
            conduct_row(head_b, k_b, third, whole_part)
            conduct_row(head_b, k_b, third + inward, top_part)

            @pl.when(jnp.logical_and(here, step == 0))
            def _():
                got(SOIL_C, 0, side, class_halo.at[side])
                got(SOIL_K, 0, side, ks.at[halo])
                sent(SOIL_C, 0, side, class_halo.at[side])
                sent(SOIL_K, 0, side, ks.at[halo])
                sent(HEAD, 0, side, tops.at[0, side, there])
                for spot in tile_spots(whole_part):
                    soil_tile(halo, spot, class_halo[side, :, spot])
                got(HEAD, 0, side, tops.at[0, side, there])

            @pl.when(jnp.logical_and(here, step == 1))
            def _():
                got(TOP_C, 0, side, class_top.at[side])
                got(TOP_K, 0, side, top_k.at[0, side])
                sent(TOP_C, 0, side, class_top.at[side])
                sent(TOP_K, 0, side, top_k.at[0, side])
                a, b, c = soil(class_top[side])
                top_soil[0, side], top_soil[1, side], top_soil[2, side] = a, b, c
                top_soil[3, side] = top_k[0, side]

            @pl.when(jnp.logical_and(here, step > 0))
            def _():
                got(TOPS, slot, side, tops.at[slot, side])

            @pl.when(here)
            def _():
                got(REST, slot, side, rest.at[slot, side])
                sent(REST, slot, side, rest.at[slot, side])

            head_a[halo, :, top_part] = tops[slot, side, there]
            head_a[halo, :, rest_part] = rest[slot, side]
            add_row(head_a.at[halo], halo_change[side, 0:1])
            beyond = tops.at[slot, side, side]
            add_row(beyond, halo_change[side, 1:2])
            top_k[1, side], _unused = conduct(
                beyond[...],
                top_soil[0, side],
                top_soil[1, side],
                top_soil[2, side],
                top_soil[3, side],
            )
            conduct_row(head_a, k_a, halo, whole_part)
            flow_rows(
                head_a,
                head_b,
                k_a,
                [own_row],
                inward,
                lambda spot: face(head_a, k_a, own_row, outer, spot),
            )
            conduct_row(head_b, k_b, own_row, whole_part)
            flow_rows(
                head_b,
                head_a,
                k_b,
                [second],
                inward,
                lambda spot: face(head_b, k_b, second, own_row, spot),
            )
            third_top = flow_rows(
                head_b,
                None,
                k_b,
                [third],
                inward,
                lambda spot: face(head_b, k_b, third, second, spot),
                part=top_part,
            )
            put_row(edge.at[side], 2, jnp.maximum(third_top, 0.0))
            put_row(edge.at[side], 1, jnp.maximum(head_a[second, :, 0:1], 0.0))

            @pl.when(jnp.logical_and(here, step == 0))
            def _():
                got(FLUX, 0, side, flux.at[0, side])
                sent(FLUX, 0, side, flux.at[0, side])

            @pl.when(jnp.logical_and(here, step > 0))
            def _():
                got(FLUX, slot, side, flux.at[slot, side, :, rest_part])
                sent(FLUX, slot, side, flux.at[slot, side, :, rest_part])

            flux[slot, side, :, top_part] = jnp.where(
                step == 0,
                flux[slot, side, :, top_part],
                (k_a[halo, :, top_part] + top_k[1, side])
                * (tops[slot, side, side] - head_a[halo, :, top_part]),
            )
            flow_rows(
                head_a, head_b, k_a, [halo], inward, lambda spot: flux[slot, side, :, spot]
            )
            conduct_row(head_b, k_b, halo, whole_part, gains=False)
            flow_rows(
                head_b,
                head_a,
                k_b,
                [own_row],
                inward,
                lambda spot: face(head_b, k_b, own_row, outer, spot),
            )
            put_row(edge.at[side], 0, jnp.maximum(head_a[own_row, :, 0:1], 0.0))

            @pl.when(here)
            def _():
                push(DEPTH, other, side, edge.at[side], edges.at[other, there])

            @pl.when(jnp.logical_and(here, going))
            def _():
                low = 1 + side * (rows - 2)
                push(
                    TOPS, other, side, head_a.at[pl.ds(low, 2), :, top_part], tops.at[other, there]
                )
                push(REST, other, side, head_a.at[own_row, :, rest_part], rest.at[other, there])

            @pl.when(going)
            def _():
                face_flux(side, rest_part)

            @pl.when(jnp.logical_and(here, going))
            def _():
                push(
                    FLUX,
                    other,
                    side,
                    flux_out.at[side, :, rest_part],
                    flux.at[other, there, :, rest_part],
                )

        both_sides(side_work, jnp.where(going, far, 1 - far))

        for row in (half, half + 1):
            conduct_row(head_b, k_b, row, rest_part)
        flow_rows(
            head_b,
            head_a,
            k_b,
            range(3, rows - 1),
            1,
            lambda spot: face(head_b, k_b, 3, 2, spot),
        )

        @pl.when(going)
        def _():
            for row in range(3, rows - 1):
                conduct_row(head_a, k_a, row, rest_part)

        @pl.when(step == 0)
        def _():
            assemble()

        for row in range(rows):
            put_row(depths, EDGE + row, jnp.maximum(head_a[row + 1, :, 0:1], 0.0))

        @pl.when(step == STEPS - 1)
        def _():
            hand_out(0, depths[own])
            for row in range(rows):
                store_out(row, range(1, tiles))

        for side in range(2):

            @pl.when(jnp.logical_and(exists(side), step > 0))
            def _():
                got(LEVEL, slot, side, level_in.at[slot, side])
                sent(LEVEL, slot, side, level_in.at[slot, side])
                beside = side * (rows + EDGE)
                levels[slot, beside : beside + EDGE] = level_in[slot, side]

        roots[...] = slope_root(maps[2], levels[slot], shifts_x)

        for side in range(2):

            @pl.when(exists(side))
            def _():
                got(DEPTH, other, side, edges.at[other, side])
                sent(DEPTH, other, side, edges.at[other, side])

        for away in range(3):
            spot = EDGE - 1 - away
            depths[spot : spot + 1] = edges[other, 0, away : away + 1]
            spot = EDGE + rows + away
            depths[spot : spot + 1] = edges[other, 1, away : away + 1]

        outflow, sediment, balance = surface(
            (maps[0], maps[1], maps[2]), roots[...], depths[...], shifts_x
        )
        change = balance(outflow)

        for side in range(2):

            @pl.when(jnp.logical_and(exists(side), going))
            def _():
                sent(TOPS, other, side, tops.at[other, side])

        for row in range(rows):
            spot = EDGE + row
            add_row(head_a.at[row + 1], change[spot : spot + 1])
        for away in range(2):
            spot = EDGE - 1 - away
            halo_change[0, away : away + 1] = change[spot : spot + 1]
            spot = EDGE + rows + away
            halo_change[1, away : away + 1] = change[spot : spot + 1]

        @pl.when(going)
        def _():
            fresh = levels[slot, own] + BED_RATE * balance(sediment)[own]
            levels[other, own] = fresh
            level_out[other, 0] = fresh[0:EDGE]
            level_out[other, 1] = fresh[rows - EDGE : rows]

        for side in range(2):

            @pl.when(jnp.logical_and(exists(side), going))
            def _():
                push(LEVEL, other, side, level_out.at[other, side], level_in.at[other, 1 - side])

        @pl.when(step == STEPS - 2)
        def _():
            hand_out(1, levels[other, own])


    for row in range(rows):
        store_out(row, range(1))
    for side in range(2):

        @pl.when(exists(side))
        def _():
            got(MAPS, 0, side, maps_y.at[:, beyond[side]])
            sent(MAPS, 0, side, maps_y.at[:, beyond[side]])

    collect(1)
    root_y = slope_root(maps_y[2], fields_y[1], shifts_y)
    collect(0)
    _unused, sediment, balance = surface(
        (maps_y[0], maps_y[1], maps_y[2]), root_y, fields_y[0], shifts_y
    )
    bed_out[...] = fields_y[1, strip_part] + BED_RATE * balance(sediment)[strip_part]


def on_device(
    pressure,
    conductivity,
    soil_class,
    vg_alpha,
    vg_shape,
    bed,
    flow_code,
    surface_soil,
    cover_class,
    ponding,
    conveyance,
    erodibility,
):
    count = lax.axis_size("tile")
    layers, rows, columns = pressure.shape
    strip, width = bed.shape
    groups = columns // LANES
    head = pressure.reshape(layers * rows, columns)
    ks = conductivity.reshape(layers * rows, columns)
    classes = soil_class.reshape(layers * rows, columns)
    vmem = pl.BlockSpec(memory_space=pltpu.VMEM)
    hbm = pl.BlockSpec(memory_space=pltpu.HBM)
    pin = lambda x: pltpu.with_memory_space_constraint(x, pltpu.HBM)
    wide = pltpu.VMEM((rows + 2, groups, layers, LANES), jnp.float32)
    dma = pltpu.SemaphoreType.DMA
    head_out, bed_out = pl.pallas_call(
        functools.partial(kernel, count, rows),
        out_shape=(
            jax.ShapeDtypeStruct((layers * rows * groups, LANES), jnp.float32),
            jax.ShapeDtypeStruct((strip, width), jnp.float32),
        ),
        in_specs=[hbm] * 12,
        out_specs=(vmem, vmem),
        scratch_shapes=[
            pltpu.VMEM((groups, layers * rows, LANES), jnp.float32),
            pltpu.VMEM((groups, layers * rows, LANES), jnp.float32),
            pltpu.VMEM((groups, layers * rows, LANES), jnp.int32),
            pltpu.SMEM(vg_alpha.shape, jnp.float32),
            pltpu.SMEM(vg_shape.shape, jnp.float32),
            pltpu.VMEM(bed.shape, jnp.float32),
            pltpu.VMEM(bed.shape, jnp.int32),
            pltpu.VMEM(bed.shape, jnp.int32),
            pltpu.VMEM(bed.shape, jnp.int32),
            pltpu.VMEM(bed.shape, jnp.int32),
            pltpu.SMEM(conveyance.shape, jnp.float32),
            pltpu.SMEM(erodibility.shape, jnp.float32),
            dma((4, max(groups, 9))),
            wide,
            wide,
            wide,
            wide,
            wide,
            wide,
            wide,
            wide,
            wide,
            pltpu.VMEM((2, 2, groups, TOP, LANES), jnp.float32),
            pltpu.VMEM((4, 2, groups, TOP, LANES), jnp.float32),
            pltpu.VMEM((rows + 2, groups, layers + TOP, LANES), jnp.float32),
            pltpu.VMEM((3, strip + 2 * TOP, width), jnp.float32),
            pltpu.VMEM((2, rows + 2 * EDGE, columns), jnp.float32),
            pltpu.VMEM((2, 2, EDGE, columns), jnp.float32),
            pltpu.VMEM((2, 2, EDGE, columns), jnp.float32),
            pltpu.VMEM((rows + 2 * EDGE, columns), jnp.float32),
            pltpu.VMEM((rows + 2 * EDGE, columns), jnp.float32),
            pltpu.VMEM((3, rows + 2 * EDGE, columns), jnp.float32),
            pltpu.VMEM((4, groups, layers, LANES), jnp.int32),
            pltpu.VMEM((2, groups, layers, LANES), jnp.int32),
            pltpu.VMEM((2, groups, TOP, LANES), jnp.int32),
            pltpu.VMEM((2, 2, 2, groups, TOP, LANES), jnp.float32),
            pltpu.VMEM((2, 2, groups, layers - TOP, LANES), jnp.float32),
            pltpu.VMEM((2, groups, layers, LANES), jnp.float32),
            pltpu.VMEM((2, 2, groups, layers, LANES), jnp.float32),
            pltpu.VMEM((2, EDGE, columns), jnp.float32),
            pltpu.VMEM((2, 2, EDGE, columns), jnp.float32),
            pltpu.VMEM((2, EDGE, columns), jnp.float32),
            pltpu.VMEM((width // EDGE + 2, EDGE, LANES), jnp.float32),
            pltpu.VMEM((count, rows // EDGE + 2, EDGE, LANES), jnp.float32),
            pltpu.VMEM((2, count, rows, LANES), jnp.float32),
            pltpu.VMEM((2, count, rows, LANES), jnp.float32),
            pltpu.VMEM((2, strip + 2 * TOP, width), jnp.float32),
            dma((KINDS, 2, 2)),
            dma((KINDS, 2, 2)),
            dma((count,)),
            dma((count,)),
            dma((2, count)),
            dma((2, count)),
        ],
        compiler_params=pltpu.CompilerParams(
            collective_id=0, has_side_effects=True, vmem_limit_bytes=40 * 1024 * 1024
        ),
    )(
        pin(head),
        pin(ks),
        pin(classes),
        pin(vg_alpha),
        pin(vg_shape),
        pin(bed),
        pin(flow_code),
        pin(surface_soil),
        pin(cover_class),
        pin(ponding),
        pin(conveyance),
        pin(erodibility),
    )
    head_out = jnp.swapaxes(head_out.reshape(layers, groups, rows, LANES), 1, 2)
    return head_out.reshape(layers, rows, columns), bed_out


def solution(mesh):
    in_specs = (
        P("member", "tile", None),
        P("member", "tile", None),
        P("member", "tile", None),
        P(),
        P(),
        P("tile", "member"),
        P("tile", "member"),
        P("tile", "member"),
        P("tile", "member"),
        P("tile", "member"),
        P(),
        P(),
    )
    out_specs = (P("member", "tile", None), P("tile", "member"))
    return jax.shard_map(
        on_device, mesh=mesh, in_specs=in_specs, out_specs=out_specs, check_vma=False
    )
```
